32 devices in a mesh: pipe: 2 (over y), dp: 16 (over z, x, core).
Axes of the slice: x: 2, y: 2, z: 4, core: 2. Of those that a mesh axis runs over, the one named last changes fastest.
Arguments:
- tokens: bfloat16 [6144, 1536], P('dp'), may hold values from -6 to 6
- cotangent: bfloat16 [6144, 1536], P('dp'), may hold values from -6 to 6
- seq_lengths: int32 [48, 8], P('dp'), may hold values from 0 to 128, as said below
- w_query: bfloat16 [2, 1536, 1536], P('pipe', 'dp'), may hold values from -0.15625 to 0.15625
- w_key: bfloat16 [2, 1536, 768], P('pipe', 'dp'), may hold values from -0.15625 to 0.15625
- w_value: bfloat16 [2, 1536, 768], P('pipe', 'dp'), may hold values from -0.15625 to 0.15625
- w_out: bfloat16 [2, 1536, 1536], P('pipe', 'dp'), may hold values from -1.25 to 1.25
- w_gate: bfloat16 [2, 1536, 4096], P('pipe', 'dp'), may hold values from -0.15625 to 0.15625
- w_up: bfloat16 [2, 1536, 4096], P('pipe', 'dp'), may hold values from -0.15625 to 0.15625
- w_down: bfloat16 [2, 4096, 1536], P('pipe', 'dp'), may hold values from -0.09375 to 0.09375
- gain_attn: bfloat16 [2, 1536], P('pipe', 'dp'), may hold values from 0.25 to 1.75
- gain_ffn: bfloat16 [2, 1536], P('pipe', 'dp'), may hold values from 0.25 to 1.75
Outputs:
- layer_outputs: bfloat16 [2, 6144, 1536], P('pipe', 'dp')
- input_grads: bfloat16 [2, 6144, 1536], P('pipe', 'dp')
- grad_query: float32 [2, 1536, 1536], P('pipe', 'dp')
- grad_key: float32 [2, 1536, 768], P('pipe', 'dp')
- grad_value: float32 [2, 1536, 768], P('pipe', 'dp')
- grad_out: float32 [2, 1536, 1536], P('pipe', 'dp')
- grad_gate: float32 [2, 1536, 4096], P('pipe', 'dp')
- grad_up: float32 [2, 1536, 4096], P('pipe', 'dp')
- grad_down: float32 [2, 4096, 1536], P('pipe', 'dp')
- grad_gain_attn: float32 [2, 1536], P('pipe', 'dp')
- grad_gain_ffn: float32 [2, 1536], P('pipe', 'dp')
The draws below stay inside these ranges and needn't reach their ends.
Inputs may be any that keep to these rules, and one draw needn't show every extreme that they name: `seq_lengths`: each row lists the lengths of the sequences packed in order into one micro-batch row of 128 slots; zeros stand for unused entries, a row's lengths sum to at most 128, and the slots after its last sequence form one more sequence.
All inputs are finite; a program needn't handle non-finite values.
Results may differ from the reference program's by a relative error of at most 0.023.
Values may be sent and summed in bfloat16 or wider, within the bound.
A program may use at most 256 MiB of HBM per device.

```python
import math
import jax
import jax.numpy as jnp
from jax import lax

D = 1536
HEADS = 16
KV_HEADS = 8
HD = 96
FF = 4096
MB_TOK = 128
SLOTS = 8
ROWS = 48
TOKENS = 6144


def draw_seq_lengths(key, part):
    fill_key = jax.random.fold_in(key, 11)
    cut_key = jax.random.fold_in(key, 12)
    pick_key = jax.random.fold_in(key, 13)
    live_counts = jax.random.randint(fill_key, (ROWS,), MB_TOK // 2, MB_TOK + 1).astype(jnp.int32)
    full_row = jax.random.randint(pick_key, (), 0, ROWS).astype(jnp.int32)
    row_ids = jnp.arange(ROWS, dtype=jnp.int32)
    live_counts = jnp.where(row_ids == full_row, MB_TOK, live_counts).astype(jnp.int32)
    cut_points = jax.random.randint(cut_key, (ROWS, SLOTS - 1), 0, MB_TOK + 1).astype(jnp.int32)
    cut_points = jnp.sort(jnp.minimum(cut_points, live_counts[:, None]), axis=-1)
    cut_points = jnp.where((row_ids == full_row)[:, None], MB_TOK, cut_points).astype(jnp.int32)
    edges = jnp.concatenate([jnp.zeros((ROWS, 1), jnp.int32), cut_points, live_counts[:, None]], axis=-1)
    return (edges[:, 1:] - edges[:, :-1]).astype(jnp.int32)


def strengthened(drawn, stream_key, source, target, shards_of, factor):
    def block_of(position):
        return (jnp.arange(drawn.shape[position]) // (drawn.shape[position] // shards_of)).reshape((-1,) + (1,) * (drawn.ndim - 1 - position))

    first = jax.random.permutation(stream_key, shards_of)[block_of(target)]
    other_side = (block_of(target) + shards_of // 2) % shards_of
    return jnp.where((block_of(source) == first) | (block_of(source) == other_side), factor * drawn, drawn)


def shard_levels(own_key, shape, split, low, high):
    loudness, own = 1.0, jax.random.fold_in(own_key, 6)
    for position, parts in split:
        heights = jnp.exp(jax.random.uniform(jax.random.fold_in(own, position), (parts,), jnp.float32, low / len(split), high / len(split)))
        loudness = loudness * jnp.repeat(heights, shape[position] // parts).reshape([-1 if axis == position else 1 for axis in range(len(shape))])
    return loudness


def normal_values(key, dims, deviation, most, pieces=(), kind=jnp.bfloat16):
    drawn = deviation * jax.random.normal(key, dims, jnp.float32)
    if pieces:
        drawn = drawn * shard_levels(key, dims, pieces, -0.22, 0.18)
    return jnp.clip(drawn, -most, most).astype(kind)


def bell_draw_with(stream_key, shape, deviation, most, shards, heavy, held_as=jnp.bfloat16):
    values = deviation * jax.random.normal(stream_key, shape, jnp.float32)
    if shards:
        values = values * shard_levels(stream_key, shape, shards, -0.22, 0.18)
    return jnp.clip(strengthened(values, jax.random.fold_in(stream_key, 3), *heavy), -most, most).astype(held_as)


def setup_inputs(seed: int = 0) -> dict:
    seeds = jax.random.split(jax.random.key(seed), 13)
    return {
        "tokens": bell_draw_with(seeds[0], (TOKENS, D), 1.0, 6.0, ((0, 16),), (0, 1, 16, 2.0)),
        "cotangent": bell_draw_with(seeds[1], (TOKENS, D), 1.0, 6.0, ((0, 16),), (0, 1, 16, 2.0)),
        "seq_lengths": draw_seq_lengths(jax.random.fold_in(seeds[12], 71), 0),
        "w_query": normal_values(seeds[3], (2, D, D), D ** -0.5, 0.15625, ((0, 2), (1, 16))),
        "w_key": normal_values(seeds[4], (2, D, KV_HEADS * HD), D ** -0.5, 0.15625, ((0, 2), (1, 16))),
        "w_value": normal_values(seeds[5], (2, D, KV_HEADS * HD), D ** -0.5, 0.15625, ((0, 2), (1, 16))),
        "w_out": normal_values(seeds[6], (2, D, D), (D // 64) ** -0.5, 1.25, ((0, 2), (1, 16))),
        "w_gate": normal_values(seeds[7], (2, D, FF), D ** -0.5, 0.15625, ((0, 2), (1, 16))),
        "w_up": normal_values(seeds[8], (2, D, FF), D ** -0.5, 0.15625, ((0, 2), (1, 16))),
        "w_down": normal_values(seeds[9], (2, FF, D), FF ** -0.5, 0.09375, ((0, 2), (1, 16))),
        "gain_attn": jnp.clip(1.0 + 0.15 * jax.random.normal(seeds[10], (2, D), jnp.float32), 0.25, 1.75).astype(jnp.bfloat16),
        "gain_ffn": jnp.clip(1.0 + 0.15 * jax.random.normal(seeds[11], (2, D), jnp.float32), 0.25, 1.75).astype(jnp.bfloat16),
    }


EPSILON = 1e-05
ROPE_BASE = 100000.0

@jax.custom_vjp
def low(v):
    return lax.optimization_barrier(v.astype(jnp.bfloat16)).astype(jnp.float32)

@jax.custom_vjp
def low_back(v):
    return v

def low_keep(v):
    return (low(v), None)

def low_pass(kept, grad):
    return (grad,)

def back_keep(v):
    return (v, None)

def back_low(kept, grad):
    return (low(grad),)
low.defvjp(low_keep, low_pass)
low_back.defvjp(back_keep, back_low)

def row_starts(lengths):
    seq_ends = jnp.cumsum(lengths, axis=-1).astype(jnp.int32)
    slot_ids = jnp.arange(MB_TOK, dtype=jnp.int32)
    reached = jnp.where(seq_ends[:, None, :] <= slot_ids[None, :, None], seq_ends[:, None, :], 0)
    return lax.optimization_barrier(jnp.max(reached, axis=-1)).astype(jnp.int32)

def rotary_tables(seg_start):
    row_length = seg_start.shape[0]
    half_dim = HD // 2
    places = (jnp.arange(row_length, dtype=jnp.int32) - seg_start).astype(jnp.float32)
    inv_freqs = jnp.exp(jnp.arange(half_dim, dtype=jnp.float32) * (-2.0 * math.log(ROPE_BASE) / HD))
    angles = places[:, None] * inv_freqs[None, :]
    return (jnp.cos(angles)[:, None, :], jnp.sin(angles)[:, None, :])

def rotate(operand, cosine, sine_part):
    half_dim = operand.shape[-1] // 2
    front_half, back_half = (operand[..., :half_dim], operand[..., half_dim:])
    return jnp.concatenate([front_half * cosine - back_half * sine_part, back_half * cosine + front_half * sine_part], axis=-1)

def attend_mask(seg_start):
    row_length = seg_start.shape[0]
    slot_ids = jnp.arange(row_length, dtype=jnp.int32)
    return (seg_start[None, :] == seg_start[:, None]) & (slot_ids[None, :] <= slot_ids[:, None])

def matmul(first_operand, second_operand):
    return jnp.dot(first_operand, second_operand, preferred_element_type=jnp.float32, precision=lax.Precision.HIGHEST)

def layer_apply(hidden, seg_start, weights, layer_index):
    w_query, w_key, w_value, w_out, w_gate, w_up, w_down, gain_attn, gain_ffn = [item[layer_index] for item in weights]
    row_length = hidden.shape[0]
    group_size = HEADS // KV_HEADS
    normed = hidden * lax.rsqrt(lax.optimization_barrier(jnp.mean(hidden * hidden, axis=-1, keepdims=True)) + EPSILON)
    attn_input = low(normed * gain_attn)
    query_proj = low_back(matmul(attn_input, w_query)).reshape(row_length, HEADS, HD)
    key_proj = low_back(matmul(attn_input, w_key)).reshape(row_length, KV_HEADS, HD)
    value_proj = low_back(matmul(attn_input, w_value)).reshape(row_length, KV_HEADS, HD)
    cosine, sine_part = rotary_tables(seg_start)
    query_rot = low(rotate(query_proj, cosine, sine_part))
    key_rot = low(rotate(key_proj, cosine, sine_part))
    value_low = low(value_proj)
    grouped = query_rot.reshape(row_length, KV_HEADS, group_size, HD)
    raw_scores = jnp.einsum('tkgd,skd->kgts', grouped, key_rot, precision=lax.Precision.HIGHEST) * (1.0 / math.sqrt(HD))
    scores = jnp.where(attend_mask(seg_start), low_back(raw_scores), -1e+30)
    attn_probs = low(jax.nn.softmax(scores, axis=-1))
    attended = jnp.einsum('kgts,skd->tkgd', attn_probs, value_low, precision=lax.Precision.HIGHEST)
    attended = low(low_back(attended.reshape(row_length, HEADS * HD)))
    mid_stream = hidden + low_back(matmul(attended, w_out))
    normed_two = mid_stream * lax.rsqrt(lax.optimization_barrier(jnp.mean(mid_stream * mid_stream, axis=-1, keepdims=True)) + EPSILON)
    ffn_input = low(normed_two * gain_ffn)
    gate_proj = low_back(matmul(ffn_input, w_gate))
    up_proj = low_back(matmul(ffn_input, w_up))
    activated = low(jax.nn.silu(gate_proj) * up_proj)
    return mid_stream + low_back(matmul(activated, w_down))

def reference(tokens, cotangent, seq_lengths, w_query, w_key, w_value, w_out, w_gate, w_up, w_down, gain_attn, gain_ffn):
    starts = row_starts(seq_lengths)
    inputs = tokens.astype(jnp.float32).reshape(ROWS, MB_TOK, D)
    cotangents = cotangent.astype(jnp.float32).reshape(ROWS, MB_TOK, D)
    weights = tuple((item.astype(jnp.float32) for item in (w_query, w_key, w_value, w_out, w_gate, w_up, w_down, gain_attn, gain_ffn)))
    probe = jnp.zeros_like(inputs)

    def forward(inputs, probe, weights):

        def row_step(carried, row_data):
            hidden, extra_term, seg_start = row_data
            front_out = layer_apply(hidden, seg_start, weights, 0)
            passed = low_back(low(front_out)) + extra_term
            back_out = layer_apply(passed, seg_start, weights, 1)
            return (carried, (front_out, back_out))
        carried, outputs = lax.scan(jax.checkpoint(row_step), jnp.zeros((), jnp.float32), (inputs, probe, starts))
        return outputs
    (fronts, backs), pullback = jax.vjp(forward, inputs, probe, weights)
    input_grad, probe_grad, weight_grads = pullback((jnp.zeros_like(fronts), cotangents))
    layer_outputs = jnp.stack([fronts, backs]).reshape(2, TOKENS, D).astype(jnp.bfloat16)
    input_grads = jnp.stack([input_grad, probe_grad]).reshape(2, TOKENS, D).astype(jnp.bfloat16)
    return (layer_outputs, input_grads, weight_grads[0], weight_grads[1], weight_grads[2], weight_grads[3], weight_grads[4], weight_grads[5], weight_grads[6], weight_grads[7], weight_grads[8])
```

```python
import functools, math
import jax
import jax.numpy as jnp
from jax import lax
from jax.experimental import pallas as pl
from jax.experimental.pallas import tpu as pltpu
from jax.sharding import PartitionSpec as P

MESH = pl.DeviceIdType.MESH
DEPTH = 4


def ring_place(dp_index, chips):
    inner = chips // DEPTH
    core = dp_index % 2
    chip = dp_index // 2
    deep = chip // inner
    spot = chip % inner
    half = inner // 2
    turn = spot + (spot // half) * (3 * half - 1 - 2 * spot)
    return turn * DEPTH + deep + (turn % 2) * (DEPTH - 1 - 2 * deep), core


def ring_device(place, core, chips):
    inner = chips // DEPTH
    half = inner // 2
    turn = place // DEPTH
    step = place % DEPTH
    deep = step + (turn % 2) * (DEPTH - 1 - 2 * step)
    spot = turn + (turn // half) * (3 * half - 1 - 2 * turn)
    return (deep * inner + spot) * 2 + core


def gather_kernel(chips, count, *refs):
    shards = refs[:count]
    wholes = refs[count : 2 * count]
    stages = refs[2 * count : 3 * count]
    ring_send, ring_recv, pair_send, pair_recv, own_pair, own_load = refs[3 * count :]
    me = lax.axis_index("dp")
    place, core = ring_place(me, chips)
    right = ring_device((place + 1) % chips, core, chips)
    left = ring_device((place + chips - 1) % chips, core, chips)
    partner = me + 1 - 2 * core
    barrier = pltpu.get_barrier_semaphore()
    for other in (right, left, partner):
        pl.semaphore_signal(barrier, inc=1, device_id={"dp": other}, device_id_type=MESH)
    pl.semaphore_wait(barrier, 3)

    def block(index, owner, way):
        rows, columns = shards[index].shape
        return wholes[index].at[
            pl.ds(pl.multiple_of(owner * rows, 8), rows), pl.ds(way * (columns // 2), columns // 2)
        ]

    def ring_copy(index, way, step, source=None):
        owner_place = (place + chips - step) % chips if way == 0 else (place + step) % chips
        owner = ring_device(owner_place, core, chips)
        target = block(index, owner, way)
        return pltpu.make_async_remote_copy(
            src_ref=target if source is None else source,
            dst_ref=target,
            send_sem=ring_send.at[index, way, step],
            recv_sem=ring_recv.at[index, way, step],
            device_id={"dp": (right, left)[way]},
            device_id_type=MESH,
        )

    def arrived(index, way, step):
        owner_place = (place + chips - step - 1) % chips if way == 0 else (place + step + 1) % chips
        owner = ring_device(owner_place, core, chips)
        target = block(index, owner, way)
        ring = pltpu.make_async_remote_copy(
            src_ref=target, dst_ref=target,
            send_sem=ring_send.at[index, way, step], recv_sem=ring_recv.at[index, way, step],
            device_id={"dp": (right, left)[way]}, device_id_type=MESH,
        )
        pair = pltpu.make_async_remote_copy(
            src_ref=target, dst_ref=target,
            send_sem=pair_send.at[index, way, step], recv_sem=pair_recv.at[index, way, step],
            device_id={"dp": partner}, device_id_type=MESH,
        )
        return ring, pair

    def own_pair_copy(index, device):
        rows = shards[index].shape[0]
        return pltpu.make_async_remote_copy(
            src_ref=shards[index],
            dst_ref=wholes[index].at[pl.ds(pl.multiple_of(device * rows, 8), rows), :],
            send_sem=own_pair.at[0, index], recv_sem=own_pair.at[1, index],
            device_id={"dp": partner}, device_id_type=MESH,
        )

    for index in range(count):
        columns = shards[index].shape[1]
        for way in range(2):
            ring_copy(index, way, 0, shards[index].at[:, pl.ds(way * (columns // 2), columns // 2)]).start()
    loads = []
    for index in range(count):
        own_pair_copy(index, me).start()
        loads.append(pltpu.make_async_copy(shards[index], stages[index], own_load.at[0, index]))
        loads[-1].start()
    stores = []
    for index in range(count):
        rows = shards[index].shape[0]
        loads[index].wait()
        stores.append(
            pltpu.make_async_copy(
                stages[index],
                wholes[index].at[pl.ds(pl.multiple_of(me * rows, 8), rows), :],
                own_load.at[1, index],
            )
        )
        stores[-1].start()

    def hop(step, carry):
        for index in range(count):
            for way in range(2):
                ring, pair = arrived(index, way, step - 1)
                ring.wait_recv()
                ring_copy(index, way, step).start()
                pair.start()
        return carry

    lax.fori_loop(1, chips - 1, hop, 0)
    for index in range(count):
        for way in range(2):
            ring, pair = arrived(index, way, chips - 2)
            ring.wait_recv()
            pair.start()

    def finish(step, carry):
        for index in range(count):
            for way in range(2):
                ring, pair = arrived(index, way, step)
                ring.wait_send()
                pair.wait_send()
                pair.wait_recv()
        return carry

    lax.fori_loop(0, chips - 1, finish, 0)
    for index in range(count):
        own_pair_copy(index, me).wait_send()
        own_pair_copy(index, partner).wait_recv()
        stores[index].wait()


def gathered(shards, chips):
    count = len(shards)
    steps = chips - 1
    return pl.pallas_call(
        functools.partial(gather_kernel, chips, count),
        out_shape=[jax.ShapeDtypeStruct((s.shape[0] * 2 * chips, s.shape[1]), s.dtype) for s in shards],
        in_specs=[pl.BlockSpec(memory_space=pl.ANY)] * count,
        out_specs=[pl.BlockSpec(memory_space=pl.ANY)] * count,
        scratch_shapes=[pltpu.VMEM(s.shape, s.dtype) for s in shards]
        + [
            pltpu.SemaphoreType.DMA((count, 2, steps)),
            pltpu.SemaphoreType.DMA((count, 2, steps)),
            pltpu.SemaphoreType.DMA((count, 2, steps)),
            pltpu.SemaphoreType.DMA((count, 2, steps)),
            pltpu.SemaphoreType.DMA((2, count)),
            pltpu.SemaphoreType.DMA((2, count)),
        ],
        compiler_params=pltpu.CompilerParams(collective_id=0, has_side_effects=True),
        name="gather_weights",
    )(*shards)


def scatter_kernel(chips, count, *refs):
    grads = refs[:count]
    sums = refs[count : 2 * count]
    lands = refs[2 * count : 3 * count]
    rest = refs[3 * count :]
    firsts = rest[:count]
    arrivals = rest[count : 2 * count]
    owns = rest[2 * count : 3 * count]
    mates = rest[3 * count : 4 * count]
    ring_send, ring_recv, pair_send, pair_recv, own_load, mate_load = rest[4 * count :]
    me = lax.axis_index("dp")
    place, core = ring_place(me, chips)
    right = ring_device((place + 1) % chips, core, chips)
    left = ring_device((place + chips - 1) % chips, core, chips)
    partner = me + 1 - 2 * core
    barrier = pltpu.get_barrier_semaphore()
    for other in (right, left, partner):
        pl.semaphore_signal(barrier, inc=1, device_id={"dp": other}, device_id_type=MESH)
    pl.semaphore_wait(barrier, 3)

    def owner_chip(way, step):
        return (place + 2 * chips - 1 - step) % chips if way == 0 else (place + 1 + step) % chips

    def pair_copy(index, way, step):
        _, _, rows, columns = arrivals[index].shape
        source = ring_device(owner_chip(way, step), 1 - core, chips)
        return pltpu.make_async_remote_copy(
            src_ref=grads[index].at[
                pl.ds(pl.multiple_of(source * rows, 8), rows), pl.ds(way * columns, columns)
            ],
            dst_ref=lands[index].at[way, step],
            send_sem=pair_send.at[index, way, step],
            recv_sem=pair_recv.at[index, way, step],
            device_id={"dp": partner},
            device_id_type=MESH,
        )

    def own_copy(index, way, step):
        _, _, rows, columns = arrivals[index].shape
        mine = ring_device(owner_chip(way, step), core, chips)
        return pltpu.make_async_copy(
            grads[index].at[
                pl.ds(pl.multiple_of(mine * rows, 8), rows), pl.ds(way * columns, columns)
            ],
            owns[index].at[step % 2, way],
            own_load.at[index, way, step % 2],
        )

    def mate_copy(index, way, step):
        return pltpu.make_async_copy(
            lands[index].at[way, step], mates[index].at[step % 2, way], mate_load.at[index, way, step % 2]
        )

    def ring_copy(index, way, step, source):
        return pltpu.make_async_remote_copy(
            src_ref=source,
            dst_ref=arrivals[index].at[way, step],
            send_sem=ring_send.at[index, way, step],
            recv_sem=ring_recv.at[index, way, step],
            device_id={"dp": (right, left)[way]},
            device_id_type=MESH,
        )

    def start_pair(step, carry):
        for index in range(count):
            for way in range(2):
                pair_copy(index, way, step).start()
        return carry

    lax.fori_loop(0, chips, start_pair, 0)

    def fetch(step):
        for index in range(count):
            for way in range(2):
                own_copy(index, way, step).start()
                pair_copy(index, way, step).wait_recv()
                mate_copy(index, way, step).start()

    def added(index, way, step, extra, target, kind):
        _, _, rows, columns = arrivals[index].shape
        own_copy(index, way, step).wait()
        mate_copy(index, way, step).wait()
        part = 32 if rows % 32 == 0 else 8
        slot = step % 2

        def piece(at, carry):
            band = pl.ds(pl.multiple_of(at * part, part), part)
            value = owns[index][slot, way, band, :].astype(jnp.float32) + mates[index][
                slot, way, band, :
            ].astype(jnp.float32)
            if extra is not None:
                value = value + extra[band, :].astype(jnp.float32)
            target[band, :] = value.astype(kind)
            return carry

        lax.fori_loop(0, rows // part, piece, 0)

    fetch(0)
    fetch(1)
    for index in range(count):
        for way in range(2):
            added(index, way, 0, None, firsts[index].at[way], firsts[index].dtype)
        for way in range(2):
            ring_copy(index, way, 0, firsts[index].at[way]).start()

    def hop(step, carry):
        fetch(step + 1)
        for index in range(count):
            for way in range(2):
                here = arrivals[index].at[way, step - 1]
                ring_copy(index, way, step - 1, here).wait_recv()
                added(index, way, step, here, here, here.dtype)
            for way in range(2):
                ring_copy(index, way, step, arrivals[index].at[way, step - 1]).start()
        return carry

    lax.fori_loop(1, chips - 1, hop, 0)
    for index in range(count):
        _, _, rows, columns = arrivals[index].shape
        for way in range(2):
            here = arrivals[index].at[way, chips - 2]
            ring_copy(index, way, chips - 2, here).wait_recv()
            added(
                index, way, chips - 1, here, sums[index].at[:, pl.ds(way * columns, columns)], jnp.float32
            )

    def finish(step, carry):
        for index in range(count):
            for way in range(2):
                ring_copy(index, way, step, firsts[index].at[way]).wait_send()
        return carry

    lax.fori_loop(0, chips - 1, finish, 0)

    def finish_pair(step, carry):
        for index in range(count):
            for way in range(2):
                pair_copy(index, way, step).wait_send()
        return carry

    lax.fori_loop(0, chips, finish_pair, 0)


def scattered(grads, chips):
    count = len(grads)
    steps = chips - 1
    half = [(g.shape[0] // (2 * chips), g.shape[1] // 2) for g in grads]
    kinds = [g.dtype for g in grads]
    outs = pl.pallas_call(
        functools.partial(scatter_kernel, chips, count),
        out_shape=[jax.ShapeDtypeStruct((r, 2 * c), jnp.float32) for r, c in half]
        + [jax.ShapeDtypeStruct((2, chips, r, c), k) for (r, c), k in zip(half, kinds)],
        in_specs=[pl.BlockSpec(memory_space=pl.ANY)] * count,
        out_specs=[pl.BlockSpec(memory_space=pltpu.VMEM)] * count
        + [pl.BlockSpec(memory_space=pl.ANY)] * count,
        scratch_shapes=[pltpu.VMEM((2, r, c), k) for (r, c), k in zip(half, kinds)]
        + [pltpu.VMEM((2, steps, r, c), k) for (r, c), k in zip(half, kinds)]
        + [pltpu.VMEM((2, 2, r, c), k) for (r, c), k in zip(half, kinds)]
        + [pltpu.VMEM((2, 2, r, c), k) for (r, c), k in zip(half, kinds)]
        + [
            pltpu.SemaphoreType.DMA((count, 2, steps)),
            pltpu.SemaphoreType.DMA((count, 2, steps)),
            pltpu.SemaphoreType.DMA((count, 2, chips)),
            pltpu.SemaphoreType.DMA((count, 2, chips)),
            pltpu.SemaphoreType.DMA((count, 2, 2)),
            pltpu.SemaphoreType.DMA((count, 2, 2)),
        ],
        compiler_params=pltpu.CompilerParams(
            collective_id=1, has_side_effects=True, vmem_limit_bytes=60 << 20
        ),
        name="scatter_grads",
    )(*grads)
    return outs[:count]


HEADS = 16
KV_HEADS = 8
HD = 96
GROUP = HEADS // KV_HEADS
EPSILON = 1e-05
ROPE_BASE = 100000.0
SCALE = 1.0 / math.sqrt(HD)
GAIN_LANES = 128


def passed_along(array, axis, by):
    count = lax.axis_size(axis)
    pairs = [(i, i + by) for i in range(count) if 0 <= i + by < count]
    return lax.ppermute(array, axis, pairs)


def row_starts(lengths, row_length):
    seq_ends = jnp.cumsum(lengths, axis=-1)
    slot_ids = jnp.arange(row_length, dtype=jnp.int32)
    reached = jnp.where(seq_ends[:, None, :] <= slot_ids[None, :, None], seq_ends[:, None, :], 0)
    return jnp.max(reached, axis=-1)


def rotary_tables(starts):
    row_length = starts.shape[1]
    half_dim = HD // 2
    places = (jnp.arange(row_length, dtype=jnp.int32)[None] - starts).astype(jnp.float32)
    inv_freqs = jnp.exp(jnp.arange(half_dim, dtype=jnp.float32) * (-2.0 * math.log(ROPE_BASE) / HD))
    angles = places[:, :, None] * inv_freqs[None, None, :]
    return (jnp.cos(angles)[:, :, None, :], jnp.sin(angles)[:, :, None, :])


def rotate(operand, cosine, sine_part):
    half_dim = operand.shape[-1] // 2
    front_half, back_half = (operand[..., :half_dim], operand[..., half_dim:])
    return jnp.concatenate(
        [front_half * cosine - back_half * sine_part, back_half * cosine + front_half * sine_part],
        axis=-1,
    )


def attend_mask(starts):
    row_length = starts.shape[1]
    slot_ids = jnp.arange(row_length, dtype=jnp.int32)
    same = starts[:, None, :] == starts[:, :, None]
    return same & (slot_ids[None, None, :] <= slot_ids[None, :, None])


def inv_rms(operand):
    return lax.rsqrt(jnp.mean(operand * operand, axis=-1, keepdims=True) + EPSILON)


def times(first_operand, second_operand):
    return jnp.dot(first_operand, second_operand, preferred_element_type=jnp.float32)


def times_transposed(first_operand, second_operand):
    return lax.dot_general(
        first_operand, second_operand, (((1,), (1,)), ((), ())), preferred_element_type=jnp.float32
    )


def across_rows(first_operand, second_operand):
    return lax.dot_general(
        first_operand, second_operand, (((0,), (0,)), ((), ())), preferred_element_type=jnp.float32
    ).astype(jnp.bfloat16)


def mixed(spec, first_operand, second_operand):
    return jnp.einsum(spec, first_operand, second_operand, preferred_element_type=jnp.float32)


def scores_of(query_rot, key_rot, mask):
    raw_scores = mixed("rtkgd,rskd->rkgts", query_rot, key_rot) * SCALE
    return jnp.where(mask[:, None, None], raw_scores, -1e30)


def forward_unit(params, input_low, tables, mask):
    w_query, w_key, w_value, w_out, w_gate, w_up, w_down, gain_one, gain_two = params
    rows, row_length = mask.shape[:2]
    tokens = input_low.shape[0]
    hidden = input_low.astype(jnp.float32)
    normed = hidden * inv_rms(hidden)
    attn_input = (normed * gain_one).astype(jnp.bfloat16)
    cosine, sine_part = tables
    query_proj = times(attn_input, w_query).reshape(rows, row_length, HEADS, HD)
    key_proj = times(attn_input, w_key).reshape(rows, row_length, KV_HEADS, HD)
    value_proj = times(attn_input, w_value).reshape(rows, row_length, KV_HEADS, HD)
    query_rot = rotate(query_proj, cosine, sine_part).astype(jnp.bfloat16)
    query_rot = query_rot.reshape(rows, row_length, KV_HEADS, GROUP, HD)
    key_rot = rotate(key_proj, cosine, sine_part).astype(jnp.bfloat16)
    value_low = value_proj.astype(jnp.bfloat16)
    scores = scores_of(query_rot, key_rot, mask)
    row_max = jnp.max(scores, axis=-1, keepdims=True)
    exp_scores = jnp.exp(scores - row_max)
    exp_total = jnp.sum(exp_scores, axis=-1, keepdims=True)
    log_total = row_max + jnp.log(exp_total)
    probs_low = (exp_scores / exp_total).astype(jnp.bfloat16)
    attended = mixed("rkgts,rskd->rtkgd", probs_low, value_low)
    attended = attended.reshape(tokens, HEADS * HD).astype(jnp.bfloat16)
    mid_stream = hidden + times(attended, w_out)
    normed_two = mid_stream * inv_rms(mid_stream)
    ffn_input = (normed_two * gain_two).astype(jnp.bfloat16)
    gate_proj = times(ffn_input, w_gate)
    up_proj = times(ffn_input, w_up)
    activated = (jax.nn.silu(gate_proj) * up_proj).astype(jnp.bfloat16)
    result = mid_stream + times(activated, w_down)
    kept_values = (
        input_low, attn_input, query_rot, key_rot, value_low, log_total, attended, mid_stream,
        ffn_input, gate_proj.astype(jnp.bfloat16), up_proj.astype(jnp.bfloat16), activated,
    )
    return (result.astype(jnp.bfloat16), kept_values)


def backward_unit(params, kept_values, tables, mask, incoming_low):
    w_query, w_key, w_value, w_out, w_gate, w_up, w_down, gain_one, gain_two = params
    (
        input_low, attn_input, query_rot, key_rot, value_low, log_total, attended, mid_stream,
        ffn_input, gate_proj, up_proj, activated,
    ) = kept_values
    gate_proj = gate_proj.astype(jnp.float32)
    up_proj = up_proj.astype(jnp.float32)
    rows, row_length = mask.shape[:2]
    tokens = input_low.shape[0]
    incoming = incoming_low.astype(jnp.float32)
    hidden = input_low.astype(jnp.float32)
    first_inv = inv_rms(hidden)
    normed = hidden * first_inv
    second_inv = inv_rms(mid_stream)
    normed_two = mid_stream * second_inv
    act_grad = times_transposed(incoming_low, w_down)
    sigmoid_gate = jax.nn.sigmoid(gate_proj)
    gate_grad = (
        act_grad * up_proj * sigmoid_gate * (1.0 + gate_proj * (1.0 - sigmoid_gate))
    ).astype(jnp.bfloat16)
    up_grad = (act_grad * gate_proj * sigmoid_gate).astype(jnp.bfloat16)
    ffn_grad = times_transposed(gate_grad, w_gate) + times_transposed(up_grad, w_up)
    gain_two_grad = jnp.sum(ffn_grad * normed_two, axis=0)
    scaled_two = ffn_grad * gain_two
    mid_grad = incoming + second_inv * (
        scaled_two - normed_two * jnp.mean(scaled_two * normed_two, axis=-1, keepdims=True)
    )
    out_grad = mid_grad.astype(jnp.bfloat16)
    attended_grad = times_transposed(out_grad, w_out).astype(jnp.bfloat16)
    attended_grad = attended_grad.reshape(rows, row_length, KV_HEADS, GROUP, HD)
    scores = scores_of(query_rot, key_rot, mask)
    attn_probs = jnp.exp(scores - log_total)
    probs_low = attn_probs.astype(jnp.bfloat16)
    prob_grad = mixed("rtkgd,rskd->rkgts", attended_grad, value_low)
    value_grad = mixed("rkgts,rtkgd->rskd", probs_low, attended_grad)
    value_grad = value_grad.reshape(tokens, KV_HEADS * HD).astype(jnp.bfloat16)
    score_grad = (
        attn_probs * (prob_grad - jnp.sum(attn_probs * prob_grad, axis=-1, keepdims=True))
    ).astype(jnp.bfloat16)
    rot_query_grad = (
        mixed("rkgts,rskd->rtkgd", score_grad, key_rot).reshape(rows, row_length, HEADS, HD) * SCALE
    )
    rot_key_grad = mixed("rkgts,rtkgd->rskd", score_grad, query_rot) * SCALE
    cosine, sine_part = tables
    query_grad = rotate(rot_query_grad, cosine, -sine_part).reshape(tokens, HEADS * HD)
    query_grad = query_grad.astype(jnp.bfloat16)
    key_grad = rotate(rot_key_grad, cosine, -sine_part).reshape(tokens, KV_HEADS * HD)
    key_grad = key_grad.astype(jnp.bfloat16)
    attn_grad = (
        times_transposed(query_grad, w_query)
        + times_transposed(key_grad, w_key)
        + times_transposed(value_grad, w_value)
    )
    gain_one_grad = jnp.sum(attn_grad * normed, axis=0)
    scaled_one = attn_grad * gain_one
    input_grad = mid_grad + first_inv * (
        scaled_one - normed * jnp.mean(scaled_one * normed, axis=-1, keepdims=True)
    )
    grad_pieces = (query_grad, key_grad, value_grad, out_grad, gate_grad, up_grad)
    return (input_grad.astype(jnp.bfloat16), grad_pieces, gain_one_grad, gain_two_grad)


def packed_gains(first, second):
    width = first.shape[-1]
    edge = ((0, 15), (0, GAIN_LANES - width))
    return jnp.concatenate([jnp.pad(first, edge), jnp.pad(second, edge)], axis=1)


def unpacked_gains(whole, width):
    kept = whole.reshape(-1, 16, 2 * GAIN_LANES)[:, 0].astype(jnp.float32)
    return kept[:, :width].reshape(-1), kept[:, GAIN_LANES : GAIN_LANES + width].reshape(-1)


def packed_gain_sums(first, second, width):
    edge = ((0, 0), (0, GAIN_LANES - width))
    joined = jnp.concatenate(
        [jnp.pad(first.reshape(-1, width), edge), jnp.pad(second.reshape(-1, width), edge)], axis=1
    )
    spread = jnp.pad(joined[:, None, :], ((0, 0), (0, 7), (0, 0)))
    return spread.reshape(-1, 2 * GAIN_LANES)


def shards(
    tokens, cotangent, seq_lengths, w_query, w_key, w_value, w_out, w_gate, w_up, w_down, gain_attn, gain_ffn,
):
    section = lax.axis_index("pipe")
    chips = lax.axis_size("dp") // 2
    row_length = tokens.shape[0] // seq_lengths.shape[0]
    starts = row_starts(seq_lengths, row_length)
    tables = rotary_tables(starts)
    mask = attend_mask(starts)
    width = gain_attn.shape[1]
    own = [w[0] for w in (w_query, w_key, w_value, w_out, w_gate, w_up, w_down)]
    wholes = gathered(own + [packed_gains(gain_attn, gain_ffn)], chips)
    params = tuple(wholes[:7]) + unpacked_gains(wholes[7], width)

    result, kept = forward_unit(params, tokens, tables, mask)
    arrived = passed_along(result, "pipe", 1)
    result, kept = lax.cond(
        section == 1,
        lambda now: forward_unit(params, arrived, tables, mask),
        lambda now: now,
        (result, kept),
    )
    back = backward_unit(params, kept, tables, mask, cotangent)
    returned = passed_along(back[0], "pipe", -1)
    back = lax.cond(
        section == 0,
        lambda now: backward_unit(params, kept, tables, mask, returned),
        lambda now: now,
        back,
    )
    incoming = jnp.where(section == 1, cotangent, returned)
    input_grad, pieces, gain_one_grad, gain_two_grad = back
    query_grad, key_grad, value_grad, out_grad, gate_grad, up_grad = pieces
    terms = [
        across_rows(kept[1], query_grad),
        across_rows(kept[1], key_grad),
        across_rows(kept[1], value_grad),
        across_rows(kept[6], out_grad),
        across_rows(kept[8], gate_grad),
        across_rows(kept[8], up_grad),
        across_rows(kept[11], incoming),
        packed_gain_sums(gain_one_grad, gain_two_grad, width),
    ]
    sums = scattered(terms, chips)
    gains = sums[7]
    return (
        result[None],
        input_grad[None],
        *(item[None] for item in sums[:7]),
        gains[:1, :width],
        gains[:1, GAIN_LANES : GAIN_LANES + width],
    )


def solution(mesh):
    in_specs = (
        P("dp", None),
        P("dp", None),
        P("dp", None),
        P("pipe", "dp", None),
        P("pipe", "dp", None),
        P("pipe", "dp", None),
        P("pipe", "dp", None),
        P("pipe", "dp", None),
        P("pipe", "dp", None),
        P("pipe", "dp", None),
        P("pipe", "dp"),
        P("pipe", "dp"),
    )
    out_specs = (
        P("pipe", "dp", None),
        P("pipe", "dp", None),
        P("pipe", "dp", None),
        P("pipe", "dp", None),
        P("pipe", "dp", None),
        P("pipe", "dp", None),
        P("pipe", "dp", None),
        P("pipe", "dp", None),
        P("pipe", "dp", None),
        P("pipe", "dp"),
        P("pipe", "dp"),
    )
    return jax.shard_map(shards, mesh=mesh, in_specs=in_specs, out_specs=out_specs, check_vma=False)
```

```python
import functools, math
import jax
import jax.numpy as jnp
from jax import lax
from jax.experimental import pallas as pl
from jax.experimental.pallas import tpu as pltpu
from jax.sharding import PartitionSpec as P

MESH = pl.DeviceIdType.MESH
DEPTH = 4


def ring_place(dp_index, chips):
    inner = chips // DEPTH
    core = dp_index % 2
    chip = dp_index // 2
    deep = chip // inner
    spot = chip % inner
    half = inner // 2
    turn = spot + (spot // half) * (3 * half - 1 - 2 * spot)
    return turn * DEPTH + deep + (turn % 2) * (DEPTH - 1 - 2 * deep), core


def ring_device(place, core, chips):
    inner = chips // DEPTH
    half = inner // 2
    turn = place // DEPTH
    step = place % DEPTH
    deep = step + (turn % 2) * (DEPTH - 1 - 2 * step)
    spot = turn + (turn // half) * (3 * half - 1 - 2 * turn)
    return (deep * inner + spot) * 2 + core


def gather_kernel(chips, count, *refs):
    shards = refs[:count]
    wholes = refs[count : 2 * count]
    stages = refs[2 * count : 3 * count]
    ring_send, ring_recv, pair_send, pair_recv, own_pair, own_load = refs[3 * count :]
    me = lax.axis_index("dp")
    place, core = ring_place(me, chips)
    right = ring_device((place + 1) % chips, core, chips)
    left = ring_device((place + chips - 1) % chips, core, chips)
    partner = me + 1 - 2 * core
    barrier = pltpu.get_barrier_semaphore()
    for other in (right, left, partner):
        pl.semaphore_signal(barrier, inc=1, device_id={"dp": other}, device_id_type=MESH)
    pl.semaphore_wait(barrier, 3)

    def block(index, owner, way):
        rows, columns = shards[index].shape
        return wholes[index].at[
            pl.ds(pl.multiple_of(owner * rows, 8), rows), pl.ds(way * (columns // 2), columns // 2)
        ]

    def ring_copy(index, way, step, source=None):
        owner_place = (place + chips - step) % chips if way == 0 else (place + step) % chips
        owner = ring_device(owner_place, core, chips)
        target = block(index, owner, way)
        return pltpu.make_async_remote_copy(
            src_ref=target if source is None else source,
            dst_ref=target,
            send_sem=ring_send.at[index, way, step],
            recv_sem=ring_recv.at[index, way, step],
            device_id={"dp": (right, left)[way]},
            device_id_type=MESH,
        )

    def arrived(index, way, step):
        owner_place = (place + chips - step - 1) % chips if way == 0 else (place + step + 1) % chips
        owner = ring_device(owner_place, core, chips)
        target = block(index, owner, way)
        ring = pltpu.make_async_remote_copy(
            src_ref=target, dst_ref=target,
            send_sem=ring_send.at[index, way, step], recv_sem=ring_recv.at[index, way, step],
            device_id={"dp": (right, left)[way]}, device_id_type=MESH,
        )
        pair = pltpu.make_async_remote_copy(
            src_ref=target, dst_ref=target,
            send_sem=pair_send.at[index, way, step], recv_sem=pair_recv.at[index, way, step],
            device_id={"dp": partner}, device_id_type=MESH,
        )
        return ring, pair

    def own_pair_copy(index, device):
        rows = shards[index].shape[0]
        return pltpu.make_async_remote_copy(
            src_ref=shards[index],
            dst_ref=wholes[index].at[pl.ds(pl.multiple_of(device * rows, 8), rows), :],
            send_sem=own_pair.at[0, index], recv_sem=own_pair.at[1, index],
            device_id={"dp": partner}, device_id_type=MESH,
        )

    for index in range(count):
        columns = shards[index].shape[1]
        for way in range(2):
            ring_copy(index, way, 0, shards[index].at[:, pl.ds(way * (columns // 2), columns // 2)]).start()
    loads = []
    for index in range(count):
        own_pair_copy(index, me).start()
        loads.append(pltpu.make_async_copy(shards[index], stages[index], own_load.at[0, index]))
        loads[-1].start()
    stores = []
    for index in range(count):
        rows = shards[index].shape[0]
        loads[index].wait()
        stores.append(
            pltpu.make_async_copy(
                stages[index],
                wholes[index].at[pl.ds(pl.multiple_of(me * rows, 8), rows), :],
                own_load.at[1, index],
            )
        )
        stores[-1].start()

    def hop(step, carry):
        for index in range(count):
            for way in range(2):
                ring, pair = arrived(index, way, step - 1)
                ring.wait_recv()
                ring_copy(index, way, step).start()
                pair.start()
        return carry

    lax.fori_loop(1, chips - 1, hop, 0)
    for index in range(count):
        for way in range(2):
            ring, pair = arrived(index, way, chips - 2)
            ring.wait_recv()
            pair.start()

    def finish(step, carry):
        for index in range(count):
            for way in range(2):
                ring, pair = arrived(index, way, step)
                ring.wait_send()
                pair.wait_send()
                pair.wait_recv()
        return carry

    lax.fori_loop(0, chips - 1, finish, 0)
    for index in range(count):
        own_pair_copy(index, me).wait_send()
        own_pair_copy(index, partner).wait_recv()
        stores[index].wait()


def gathered(shards, chips):
    count = len(shards)
    steps = chips - 1
    return pl.pallas_call(
        functools.partial(gather_kernel, chips, count),
        out_shape=[jax.ShapeDtypeStruct((s.shape[0] * 2 * chips, s.shape[1]), s.dtype) for s in shards],
        in_specs=[pl.BlockSpec(memory_space=pl.ANY)] * count,
        out_specs=[pl.BlockSpec(memory_space=pl.ANY)] * count,
        scratch_shapes=[pltpu.VMEM(s.shape, s.dtype) for s in shards]
        + [
            pltpu.SemaphoreType.DMA((count, 2, steps)),
            pltpu.SemaphoreType.DMA((count, 2, steps)),
            pltpu.SemaphoreType.DMA((count, 2, steps)),
            pltpu.SemaphoreType.DMA((count, 2, steps)),
            pltpu.SemaphoreType.DMA((2, count)),
            pltpu.SemaphoreType.DMA((2, count)),
        ],
        compiler_params=pltpu.CompilerParams(collective_id=0, has_side_effects=True),
        name="gather_weights",
    )(*shards)


def scatter_kernel(chips, count, *refs):
    grads = refs[:count]
    sums = refs[count : 2 * count]
    lands = refs[2 * count : 3 * count]
    rest = refs[3 * count :]
    firsts = rest[:count]
    arrivals = rest[count : 2 * count]
    owns = rest[2 * count : 3 * count]
    mates = rest[3 * count : 4 * count]
    ring_send, ring_recv, pair_send, pair_recv, own_load, mate_load = rest[4 * count :]
    me = lax.axis_index("dp")
    place, core = ring_place(me, chips)
    right = ring_device((place + 1) % chips, core, chips)
    left = ring_device((place + chips - 1) % chips, core, chips)
    partner = me + 1 - 2 * core
    barrier = pltpu.get_barrier_semaphore()
    for other in (right, left, partner):
        pl.semaphore_signal(barrier, inc=1, device_id={"dp": other}, device_id_type=MESH)
    pl.semaphore_wait(barrier, 3)

    def owner_chip(way, step):
        return (place + 2 * chips - 1 - step) % chips if way == 0 else (place + 1 + step) % chips

    def pair_copy(index, way, step):
        _, _, rows, columns = arrivals[index].shape
        source = ring_device(owner_chip(way, step), 1 - core, chips)
        return pltpu.make_async_remote_copy(
            src_ref=grads[index].at[
                pl.ds(pl.multiple_of(source * rows, 8), rows), pl.ds(way * columns, columns)
            ],
            dst_ref=lands[index].at[way, step],
            send_sem=pair_send.at[index, way, step],
            recv_sem=pair_recv.at[index, way, step],
            device_id={"dp": partner},
            device_id_type=MESH,
        )

    def own_copy(index, way, step):
        _, _, rows, columns = arrivals[index].shape
        mine = ring_device(owner_chip(way, step), core, chips)
        return pltpu.make_async_copy(
            grads[index].at[
                pl.ds(pl.multiple_of(mine * rows, 8), rows), pl.ds(way * columns, columns)
            ],
            owns[index].at[step % 2, way],
            own_load.at[index, way, step % 2],
        )

    def mate_copy(index, way, step):
        return pltpu.make_async_copy(
            lands[index].at[way, step], mates[index].at[step % 2, way], mate_load.at[index, way, step % 2]
        )

    def ring_copy(index, way, step, source):
        return pltpu.make_async_remote_copy(
            src_ref=source,
            dst_ref=arrivals[index].at[way, step],
            send_sem=ring_send.at[index, way, step],
            recv_sem=ring_recv.at[index, way, step],
            device_id={"dp": (right, left)[way]},
            device_id_type=MESH,
        )

    def start_pair(step, carry):
        for index in range(count):
            for way in range(2):
                pair_copy(index, way, step).start()
        return carry

    lax.fori_loop(0, chips, start_pair, 0)

    def fetch(step):
        for index in range(count):
            for way in range(2):
                own_copy(index, way, step).start()
                pair_copy(index, way, step).wait_recv()
                mate_copy(index, way, step).start()

    def added(index, way, step, extra, target, kind):
        _, _, rows, columns = arrivals[index].shape
        own_copy(index, way, step).wait()
        mate_copy(index, way, step).wait()
        part = 32 if rows % 32 == 0 else 8
        slot = step % 2

        def piece(at, carry):
            band = pl.ds(pl.multiple_of(at * part, part), part)
            value = owns[index][slot, way, band, :].astype(jnp.float32) + mates[index][
                slot, way, band, :
            ].astype(jnp.float32)
            if extra is not None:
                value = value + extra[band, :].astype(jnp.float32)
            target[band, :] = value.astype(kind)
            return carry

        lax.fori_loop(0, rows // part, piece, 0)

    fetch(0)
    fetch(1)
    for index in range(count):
        for way in range(2):
            added(index, way, 0, None, firsts[index].at[way], firsts[index].dtype)
        for way in range(2):
            ring_copy(index, way, 0, firsts[index].at[way]).start()

    def hop(step, carry):
        fetch(step + 1)
        for index in range(count):
            for way in range(2):
                here = arrivals[index].at[way, step - 1]
                ring_copy(index, way, step - 1, here).wait_recv()
                added(index, way, step, here, here, here.dtype)
            for way in range(2):
                ring_copy(index, way, step, arrivals[index].at[way, step - 1]).start()
        return carry

    lax.fori_loop(1, chips - 1, hop, 0)
    for index in range(count):
        _, _, rows, columns = arrivals[index].shape
        for way in range(2):
            here = arrivals[index].at[way, chips - 2]
            ring_copy(index, way, chips - 2, here).wait_recv()
            added(
                index, way, chips - 1, here, sums[index].at[:, pl.ds(way * columns, columns)], jnp.float32
            )

    def finish(step, carry):
        for index in range(count):
            for way in range(2):
                ring_copy(index, way, step, firsts[index].at[way]).wait_send()
        return carry

    lax.fori_loop(0, chips - 1, finish, 0)

    def finish_pair(step, carry):
        for index in range(count):
            for way in range(2):
                pair_copy(index, way, step).wait_send()
        return carry

    lax.fori_loop(0, chips, finish_pair, 0)


def scattered(grads, chips):
    count = len(grads)
    steps = chips - 1
    half = [(g.shape[0] // (2 * chips), g.shape[1] // 2) for g in grads]
    kinds = [g.dtype for g in grads]
    outs = pl.pallas_call(
        functools.partial(scatter_kernel, chips, count),
        out_shape=[jax.ShapeDtypeStruct((r, 2 * c), jnp.float32) for r, c in half]
        + [jax.ShapeDtypeStruct((2, chips, r, c), k) for (r, c), k in zip(half, kinds)],
        in_specs=[pl.BlockSpec(memory_space=pl.ANY)] * count,
        out_specs=[pl.BlockSpec(memory_space=pltpu.VMEM)] * count
        + [pl.BlockSpec(memory_space=pl.ANY)] * count,
        scratch_shapes=[pltpu.VMEM((2, r, c), k) for (r, c), k in zip(half, kinds)]
        + [pltpu.VMEM((2, steps, r, c), k) for (r, c), k in zip(half, kinds)]
        + [pltpu.VMEM((2, 2, r, c), k) for (r, c), k in zip(half, kinds)]
        + [pltpu.VMEM((2, 2, r, c), k) for (r, c), k in zip(half, kinds)]
        + [
            pltpu.SemaphoreType.DMA((count, 2, steps)),
            pltpu.SemaphoreType.DMA((count, 2, steps)),
            pltpu.SemaphoreType.DMA((count, 2, chips)),
            pltpu.SemaphoreType.DMA((count, 2, chips)),
            pltpu.SemaphoreType.DMA((count, 2, 2)),
            pltpu.SemaphoreType.DMA((count, 2, 2)),
        ],
        compiler_params=pltpu.CompilerParams(
            collective_id=1, has_side_effects=True, vmem_limit_bytes=60 << 20
        ),
        name="scatter_grads",
    )(*grads)
    return outs[:count]


HEADS = 16
KV_HEADS = 8
HD = 96
EPSILON = 1e-05
ROPE_BASE = 100000.0
SCALE = 1.0 / math.sqrt(HD)
GAIN_LANES = 128


def row_starts(lengths, row_length):
    seq_ends = jnp.cumsum(lengths, axis=-1)
    slot_ids = jnp.arange(row_length, dtype=jnp.int32)
    reached = jnp.where(seq_ends[:, None, :] <= slot_ids[None, :, None], seq_ends[:, None, :], 0)
    return jnp.max(reached, axis=-1)


def packed_gains(first, second):
    width = first.shape[-1]
    edge = ((0, 15), (0, GAIN_LANES - width))
    return jnp.concatenate([jnp.pad(first, edge), jnp.pad(second, edge)], axis=1)


def unpacked_gains(whole, width):
    kept = whole.reshape(-1, 16, 2 * GAIN_LANES)[:, 0].astype(jnp.float32)
    return kept[:, :width].reshape(1, -1), kept[:, GAIN_LANES : GAIN_LANES + width].reshape(1, -1)


def packed_gain_sums(first, second, width):
    edge = ((0, 0), (0, GAIN_LANES - width))
    joined = jnp.concatenate(
        [jnp.pad(first.reshape(-1, width), edge), jnp.pad(second.reshape(-1, width), edge)], axis=1
    )
    spread = jnp.pad(joined[:, None, :], ((0, 0), (0, 7), (0, 0)))
    return spread.reshape(-1, 2 * GAIN_LANES)


def spread_heads(tile, lane):
    first, second, third = tile[:, :128], tile[:, 128:256], tile[:, 256:384]
    return (
        first,
        jnp.where(lane < 32, pltpu.roll(first, 32, 1), pltpu.roll(second, 32, 1)),
        jnp.where(lane < 64, pltpu.roll(second, 64, 1), pltpu.roll(third, 64, 1)),
        pltpu.roll(third, 96, 1),
    )


def joined_heads(heads, lane):
    one, two, three = pltpu.roll(heads[1], 96, 1), pltpu.roll(heads[2], 64, 1), pltpu.roll(heads[3], 32, 1)
    return (
        jnp.where(lane < 96, heads[0], one),
        jnp.where(lane < 64, one, two),
        jnp.where(lane < 32, two, three),
    )


def turned(head, cosine, fore, aft):
    return head * cosine + pltpu.roll(head, 80, 1) * fore + pltpu.roll(head, 48, 1) * aft


def streamed(count, depth, copies, use):
    def body(j, carry):
        @pl.when(j + depth - 1 < count)
        def _():
            for copy in copies(j + depth - 1, (j + depth - 1) % depth):
                copy.start()

        for copy in copies(j, j % depth):
            copy.wait()
        use(j, j % depth)
        return carry

    lax.fori_loop(0, count, body, 0)


def lead(count, depth, copies):
    for j in range(min(depth - 1, count)):
        for copy in copies(j, j % depth):
            copy.start()


def normal_rows(source, target, gain, rows):
    band_rows = 64

    def body(i, carry):
        band = pl.ds(pl.multiple_of(i * band_rows, band_rows), band_rows)
        value = source[band, :].astype(jnp.float32)
        scale = lax.rsqrt(jnp.mean(value * value, axis=-1, keepdims=True) + EPSILON)
        target[band, :] = ((value * scale) * gain[...]).astype(jnp.bfloat16)
        return carry

    lax.fori_loop(0, rows // band_rows, body, 0)


def head_lane():
    return lax.broadcasted_iota(jnp.int32, (MB, 128), 1)


MB = 128
FWD_KEPT = ("attn_input", "queries", "keys", "values", "probs", "attended", "mid", "ffn_input", "gate", "up", "activated")


def forward_kernel(rows, *refs):
    (tokens, seg_column, seg_row, cosine, fore, aft, gain_one, gain_two,
     w_query, w_key, w_value, w_out, w_gate, w_up, w_down,
     out_ref, source_ref, attn_input_o, queries_o, keys_o, values_o, probs_o, attended_o, mid_o, ffn_input_o, gate_o, up_o, activated_o,
     source, result, attn_input, queries, keys, values, probs, attended, mid, ffn_input, gate, up, activated,
     square, pair_slot, tall,
     square_sem, pair_sem, tall_sem, keep_sem, load_sem, send_sem, recv_sem) = refs
    section = lax.axis_index("pipe")
    width = tokens.shape[1]
    inner = w_gate.shape[1]
    kv_width = w_key.shape[1]
    micro = rows // MB
    barrier = pltpu.get_barrier_semaphore()
    pl.semaphore_signal(barrier, inc=1, device_id={"pipe": 1 - section}, device_id_type=MESH)
    pl.semaphore_wait(barrier, 1)

    def pass_on(part):
        band = pl.ds(part * MB, MB)
        return pltpu.make_async_remote_copy(
            src_ref=result.at[band, :], dst_ref=source.at[band, :],
            send_sem=send_sem.at[part], recv_sem=recv_sem.at[part],
            device_id={"pipe": 1 - section}, device_id_type=MESH,
        )

    step = 768
    per_query = width // step
    per_kv = kv_width // step

    def qkv_copies(j):
        if j < per_query:
            weight, at = w_query, j
        elif j < per_query + per_kv:
            weight, at = w_key, j - per_query
        else:
            weight, at = w_value, j - per_query - per_kv
        return pltpu.make_async_copy(
            weight.at[:, pl.ds(at * step, step)], square.at[j % 4], square_sem.at[j % 4]
        )

    def out_copy(j):
        return pltpu.make_async_copy(
            w_out.at[:, pl.ds(j * step, step)], square.at[j % 4], square_sem.at[j % 4]
        )

    wide = 1024

    def ffn_copies(j, slot):
        column = pl.ds(pl.multiple_of(j * wide, wide), wide)
        return (
            pltpu.make_async_copy(w_gate.at[:, column], pair_slot.at[slot, 0], pair_sem.at[slot, 0]),
            pltpu.make_async_copy(w_up.at[:, column], pair_slot.at[slot, 1], pair_sem.at[slot, 1]),
        )

    narrow = 512

    def down_copies(j, slot):
        column = pl.ds(pl.multiple_of(j * narrow, narrow), narrow)
        return (pltpu.make_async_copy(w_down.at[:, column], tall.at[slot], tall_sem.at[slot]),)

    count_qkv = per_query + 2 * per_kv
    for j in range(4):
        qkv_copies(j).start()
    lead(inner // wide, 2, ffn_copies)
    lead(width // narrow, 2, down_copies)

    @pl.when(section == 0)
    def _():
        load = pltpu.make_async_copy(tokens, source, load_sem)
        load.start()
        load.wait()

    @pl.when(section == 1)
    def _():
        for part in range(micro):
            pass_on(part).wait_recv()

    kept = []

    def keep(index, here, there):
        copy = pltpu.make_async_copy(here, there, keep_sem.at[index])
        copy.start()
        kept.append(copy)

    keep(12, source, source_ref)
    normal_rows(source, attn_input, gain_one, rows)
    keep(0, attn_input, attn_input_o)
    lane = lax.broadcasted_iota(jnp.int32, (rows, 128), 1)

    def project(j):
        qkv_copies(j).wait()
        value = jnp.dot(attn_input[...], square[j % 4], preferred_element_type=jnp.float32)
        if j + 4 < count_qkv:
            qkv_copies(j + 4).start()
        elif j + 4 - count_qkv < width // step:
            pass
        return value

    for j in range(count_qkv):
        value = project(j)
        for part in range(2):
            heads = spread_heads(value[:, part * 384 : part * 384 + 384], lane)
            for k in range(4):
                if j < per_query + per_kv:
                    low = turned(heads[k], cosine[...], fore[...], aft[...]).astype(jnp.bfloat16)
                else:
                    low = jnp.where(lane < HD, heads[k], 0.0).astype(jnp.bfloat16)
                if j < per_query:
                    at, target = j * 8 + part * 4 + k, queries
                elif j < per_query + per_kv:
                    at, target = (j - per_query) * 8 + part * 4 + k, keys
                else:
                    at, target = (j - per_query - per_kv) * 8 + part * 4 + k, values
                target[:, pl.ds(at * 128, 128)] = low
    for j in range(width // step):
        out_copy(j).start()
    keep(1, queries, queries_o)
    keep(2, keys, keys_o)
    keep(3, values, values_o)

    def attend(at, carry):
        row = at // 2
        quad = at % 2
        band = pl.ds(pl.multiple_of(row * MB, MB), MB)
        slot_i = lax.broadcasted_iota(jnp.int32, (2 * MB, MB), 0)
        slot_i = jnp.where(slot_i >= MB, slot_i - MB, slot_i)
        slot_j = lax.broadcasted_iota(jnp.int32, (2 * MB, MB), 1)
        column = seg_column[band, :]
        same = jnp.concatenate([column, column], axis=0) == seg_row[pl.ds(row, 1), :]
        mask = same & (slot_j <= slot_i)
        small = head_lane()
        outs = []
        for k in range(4):
            kv = pl.ds(pl.multiple_of((quad * 4 + k) * 128, 128), 128)
            pair = quad * 8 + 2 * k
            query = jnp.concatenate(
                [
                    queries[band, pl.ds(pl.multiple_of(pair * 128, 128), 128)],
                    queries[band, pl.ds(pl.multiple_of((pair + 1) * 128, 128), 128)],
                ],
                axis=0,
            )
            scores = lax.dot_general(
                query, keys[band, kv], (((1,), (1,)), ((), ())), preferred_element_type=jnp.float32
            ) * SCALE
            scores = jnp.where(mask, scores, -1e30)
            high = jnp.max(scores, axis=-1, keepdims=True)
            grown = jnp.exp(scores - high)
            low = (grown / jnp.sum(grown, axis=-1, keepdims=True)).astype(jnp.bfloat16)
            place = pl.ds(pl.multiple_of((at * 4 + k) * 2 * MB, 2 * MB), 2 * MB)
            probs[place, :] = low
            out = jnp.dot(low, values[band, kv], preferred_element_type=jnp.float32)
            outs += [out[:MB], out[MB:]]
        for part in range(2):
            for c, piece in enumerate(joined_heads(outs[part * 4 : part * 4 + 4], small)):
                column = pl.ds(pl.multiple_of(quad * 768 + part * 384 + c * 128, 128), 128)
                attended[band, column] = piece.astype(jnp.bfloat16)
        return carry

    lax.fori_loop(0, 2 * micro, attend, 0)
    keep(4, probs, probs_o)
    keep(5, attended, attended_o)
    for j in range(width // step):
        out_copy(j).wait()
        column = pl.ds(j * step, step)
        mid[:, column] = source[:, column].astype(jnp.float32) + jnp.dot(
            attended[...], square[j % 4], preferred_element_type=jnp.float32
        )
    keep(6, mid, mid_o)
    normal_rows(mid, ffn_input, gain_two, rows)
    keep(7, ffn_input, ffn_input_o)

    def expand(j, slot):
        column = pl.ds(pl.multiple_of(j * wide, wide), wide)
        gate_part = jnp.dot(ffn_input[...], pair_slot[slot, 0], preferred_element_type=jnp.float32)
        up_part = jnp.dot(ffn_input[...], pair_slot[slot, 1], preferred_element_type=jnp.float32)
        gate[:, column] = gate_part.astype(jnp.bfloat16)
        up[:, column] = up_part.astype(jnp.bfloat16)
        activated[:, column] = (gate_part / (1.0 + jnp.exp(-gate_part)) * up_part).astype(jnp.bfloat16)

    streamed(inner // wide, 2, ffn_copies, expand)
    keep(8, gate, gate_o)
    keep(9, up, up_o)
    keep(10, activated, activated_o)

    def contract(j, slot):
        column = pl.ds(pl.multiple_of(j * narrow, narrow), narrow)
        value = mid[:, column] + jnp.dot(activated[...], tall[slot], preferred_element_type=jnp.float32)
        result[:, column] = value.astype(jnp.bfloat16)

    streamed(width // narrow, 2, down_copies, contract)
    keep(11, result, out_ref)

    @pl.when(section == 0)
    def _():
        for part in range(micro):
            pass_on(part).start()
        for part in range(micro):
            pass_on(part).wait_send()

    for copy in kept:
        copy.wait()


def forward_call(tokens, starts, tables, gain_one, gain_two, weights):
    rows, width = tokens.shape
    micro = rows // MB
    inner = weights[4].shape[1]
    kv_width = weights[1].shape[1]
    low, full = jnp.bfloat16, jnp.float32
    S = jax.ShapeDtypeStruct
    kept = [
        S((rows, width), low), S((rows, HEADS * 128), low), S((rows, KV_HEADS * 128), low), S((rows, KV_HEADS * 128), low),
        S((micro * HEADS * MB, MB), low), S((rows, width), low), S((rows, width), full), S((rows, width), low),
        S((rows, inner), low), S((rows, inner), low), S((rows, inner), low),
    ]
    anywhere = pl.BlockSpec(memory_space=pl.ANY)
    local = pl.BlockSpec(memory_space=pltpu.VMEM)
    square = 1536 // 2
    outs = pl.pallas_call(
        functools.partial(forward_kernel, rows),
        out_shape=[S((rows, width), low), S((rows, width), low)] + kept,
        in_specs=[anywhere] + [local] * 7 + [anywhere] * 7,
        out_specs=[anywhere] * (2 + len(kept)),
        scratch_shapes=[pltpu.VMEM((rows, width), low), pltpu.VMEM((rows, width), low)]
        + [pltpu.VMEM(k.shape, k.dtype) for k in kept]
        + [
            pltpu.VMEM((4, width, square), low),
            pltpu.VMEM((2, 2, width, 1024), low),
            pltpu.VMEM((2, inner, 512), low),
            pltpu.SemaphoreType.DMA((4,)),
            pltpu.SemaphoreType.DMA((2, 2)),
            pltpu.SemaphoreType.DMA((2,)),
            pltpu.SemaphoreType.DMA((13,)),
            pltpu.SemaphoreType.DMA,
            pltpu.SemaphoreType.DMA((micro,)),
            pltpu.SemaphoreType.DMA((micro,)),
        ],
        compiler_params=pltpu.CompilerParams(collective_id=2, has_side_effects=True, vmem_limit_bytes=63 << 20),
        name="forward_layers",
    )(tokens, starts.reshape(rows, 1), starts, *tables, gain_one, gain_two, *weights)
    return outs[0], outs[1], outs[2:]


def padded_tables(starts):
    places = (jnp.arange(starts.shape[1], dtype=jnp.int32)[None] - starts).astype(jnp.float32).reshape(-1, 1)
    lanes = jnp.arange(128, dtype=jnp.int32)
    half = HD // 2
    inv_freqs = jnp.exp((lanes % half).astype(jnp.float32) * (-2.0 * math.log(ROPE_BASE) / HD))
    angles = places * inv_freqs[None]
    cosine, sine = jnp.cos(angles), jnp.sin(angles)
    return (
        jnp.where(lanes < HD, cosine, 0.0),
        jnp.where(lanes < half, -sine, 0.0),
        jnp.where((lanes >= half) & (lanes < HD), sine, 0.0),
    )


def dot_nt(first, second):
    return lax.dot_general(first, second, (((1,), (1,)), ((), ())), preferred_element_type=jnp.float32)


def dot_tn(first, second):
    return lax.dot_general(first, second, (((0,), (0,)), ((), ())), preferred_element_type=jnp.float32)


def norm_back(grad, stream, gain, upper, target, low_target, gain_sum, rows):
    band_rows = 32
    gain_sum[...] = jnp.zeros_like(gain_sum)

    def body(i, carry):
        band = pl.ds(pl.multiple_of(i * band_rows, band_rows), band_rows)
        value = stream[band, :].astype(jnp.float32)
        scale = lax.rsqrt(jnp.mean(value * value, axis=-1, keepdims=True) + EPSILON)
        normed = value * scale
        term = grad[band, :] * normed
        gain_sum[...] += term.reshape(band_rows // 8, 8, term.shape[1]).sum(axis=0)
        inner_mean = jnp.mean(term * gain[...], axis=-1, keepdims=True)
        out = upper[band, :].astype(jnp.float32) + scale * (grad[band, :] * gain[...] - normed * inner_mean)
        if target is not None:
            target[band, :] = out
        low_target[band, :] = out.astype(jnp.bfloat16)
        return carry

    lax.fori_loop(0, rows // band_rows, body, 0)


def backward_kernel(rows, *refs):
    (cotangent, cosine, fore, aft, gain_one, gain_two,
     w_query, w_key, w_value, w_out, w_gate, w_up, w_down,
     source_i, attn_input_i, queries_i, keys_i, values_i, probs_i, attended_i, mid_i, ffn_input_i, gate_i, up_i, activated_i,
     out_ref, gain_one_o, gain_two_o, g_query, g_key, g_value, g_out, g_gate, g_up, g_down,
     incoming, passed, activated, ffn_input, attn_input, attended, source, mid, probs, queries, keys, values,
     gate_grad, up_grad, stream_grad, out_grad, heads_grad, query_grad, key_grad, value_grad,
     gate_slot, flat, kv_slot, pair_slot, flat_stage, wide_stage,
     gate_sem, flat_sem, kv_sem, pair_sem, flat_out, wide_out, load_sem, send_sem, recv_sem) = refs
    section = lax.axis_index("pipe")
    width = cotangent.shape[1]
    inner = w_gate.shape[1]
    kv_width = w_key.shape[1]
    micro = rows // MB
    barrier = pltpu.get_barrier_semaphore()
    pl.semaphore_signal(barrier, inc=1, device_id={"pipe": 1 - section}, device_id_type=MESH)
    pl.semaphore_wait(barrier, 1)

    def pass_on(part):
        band = pl.ds(part * MB, MB)
        return pltpu.make_async_remote_copy(
            src_ref=passed.at[band, :], dst_ref=incoming.at[band, :],
            send_sem=send_sem.at[part], recv_sem=recv_sem.at[part],
            device_id={"pipe": 1 - section}, device_id_type=MESH,
        )

    def loading(index, there, here):
        copy = pltpu.make_async_copy(there, here, load_sem.at[index])
        copy.start()
        return copy

    act_load = loading(0, activated_i, activated)
    mid_load = loading(1, mid_i, mid)
    rest_loads = [
        loading(2 + i, there, here)
        for i, (there, here) in enumerate(
            ((probs_i, probs), (queries_i, queries), (keys_i, keys), (values_i, values),
             (source_i, source), (ffn_input_i, ffn_input), (attn_input_i, attn_input), (attended_i, attended))
        )
    ]
    step = 512

    def flat_copy(weight, j, slot):
        return pltpu.make_async_copy(
            weight.at[pl.ds(pl.multiple_of(j * step, step), step), :], flat.at[slot], flat_sem.at[slot]
        )

    def down_copies(j, slot):
        column = pl.ds(pl.multiple_of(j * step, step), step)
        return (
            flat_copy(w_down, j, slot),
            pltpu.make_async_copy(gate_i.at[:, column], gate_slot.at[slot, 0], gate_sem.at[slot, 0]),
            pltpu.make_async_copy(up_i.at[:, column], gate_slot.at[slot, 1], gate_sem.at[slot, 1]),
        )

    def out_copies(j, slot):
        return (flat_copy(w_out, j, slot),)

    def qkv_copies(j, slot):
        band = pl.ds(pl.multiple_of(j * step, step), step)
        return (
            flat_copy(w_query, j, slot),
            pltpu.make_async_copy(w_key.at[band, :], kv_slot.at[slot, 0], kv_sem.at[slot, 0]),
            pltpu.make_async_copy(w_value.at[band, :], kv_slot.at[slot, 1], kv_sem.at[slot, 1]),
        )

    short = 256

    def ffn_copies(j, slot):
        band = pl.ds(pl.multiple_of(j * short, short), short)
        return (
            pltpu.make_async_copy(w_gate.at[band, :], pair_slot.at[slot, 0], pair_sem.at[slot, 0]),
            pltpu.make_async_copy(w_up.at[band, :], pair_slot.at[slot, 1], pair_sem.at[slot, 1]),
        )

    lead(inner // step, 3, down_copies)
    lead(width // short, 2, ffn_copies)

    @pl.when(section == 1)
    def _():
        load = loading(10, cotangent, incoming)
        load.wait()

    @pl.when(section == 0)
    def _():
        for part in range(micro):
            pass_on(part).wait_recv()

    def staged(left, left_step, right, stage, sems, targets):
        count = left.shape[1] // left_step
        columns = right.shape[1]

        def put(j, slot):
            band = pl.ds(pl.multiple_of(j * left_step, left_step), left_step)
            return pltpu.make_async_copy(
                stage.at[slot, :, pl.ds(0, columns)], targets.at[band, :], sems.at[slot]
            )

        def body(j, carry):
            @pl.when(j >= 2)
            def _():
                put(j - 2, j % 2).wait()

            column = pl.ds(pl.multiple_of(j * left_step, left_step), left_step)
            stage[j % 2, :, pl.ds(0, columns)] = dot_tn(left[:, column], right[...]).astype(jnp.bfloat16)
            put(j, j % 2).start()
            return carry

        lax.fori_loop(0, count, body, 0)
        for j in range(max(0, count - 2), count):
            put(j, j % 2).wait()

    def contract_back(j, slot):
        column = pl.ds(pl.multiple_of(j * step, step), step)
        act_grad = dot_nt(incoming[...], flat[slot])
        gate = gate_slot[slot, 0].astype(jnp.float32)
        up = gate_slot[slot, 1].astype(jnp.float32)
        sigmoid = 1.0 / (1.0 + jnp.exp(-gate))
        gate_grad[:, column] = (act_grad * up * sigmoid * (1.0 + gate * (1.0 - sigmoid))).astype(jnp.bfloat16)
        up_grad[:, column] = (act_grad * gate * sigmoid).astype(jnp.bfloat16)

    streamed(inner // step, 3, down_copies, contract_back)
    lead(width // step, 3, out_copies)

    def expand_back(j, slot):
        column = pl.ds(pl.multiple_of(j * short, short), short)
        stream_grad[:, column] = dot_nt(gate_grad[...], pair_slot[slot, 0]) + dot_nt(up_grad[...], pair_slot[slot, 1])

    streamed(width // short, 2, ffn_copies, expand_back)
    mid_load.wait()
    norm_back(stream_grad, mid, gain_two, incoming, mid, out_grad, gain_two_o, rows)
    lane = lax.broadcasted_iota(jnp.int32, (rows, 128), 1)

    def attended_back(j, slot):
        column = pl.ds(pl.multiple_of(j * step, step), step)
        stream_grad[:, column] = dot_nt(out_grad[...], flat[slot])

    streamed(width // step, 3, out_copies, attended_back)
    lead(width // step, 3, qkv_copies)
    for part in range(width // 384):
        tile = stream_grad[:, pl.ds(part * 384, 384)]
        for k, head in enumerate(spread_heads(tile, lane)):
            heads_grad[:, pl.ds((part * 4 + k) * 128, 128)] = jnp.where(lane < HD, head, 0.0).astype(jnp.bfloat16)
    for copy in rest_loads:
        copy.wait()

    def attend_back(at, carry):
        row = at // 2
        quad = at % 2
        band = pl.ds(pl.multiple_of(row * MB, MB), MB)
        small = head_lane()
        table = (cosine[band, :], fore[band, :], aft[band, :])

        def unturned(head):
            return head * table[0] - pltpu.roll(head, 80, 1) * table[1] - pltpu.roll(head, 48, 1) * table[2]

        query_parts, key_parts, value_parts = [], [], []
        for k in range(4):
            kv = pl.ds(pl.multiple_of((quad * 4 + k) * 128, 128), 128)
            pair = quad * 8 + 2 * k
            first = pl.ds(pl.multiple_of(pair * 128, 128), 128)
            second = pl.ds(pl.multiple_of((pair + 1) * 128, 128), 128)
            query = jnp.concatenate([queries[band, first], queries[band, second]], axis=0)
            out = jnp.concatenate([heads_grad[band, first], heads_grad[band, second]], axis=0)
            low = probs[pl.ds(pl.multiple_of((at * 4 + k) * 2 * MB, 2 * MB), 2 * MB), :]
            prob_grad = dot_nt(out, values[band, kv])
            value_parts.append(dot_tn(low, out))
            full = low.astype(jnp.float32)
            score = full * (prob_grad - jnp.sum(full * prob_grad, axis=-1, keepdims=True))
            score = score.astype(jnp.bfloat16)
            back = jnp.dot(score, keys[band, kv], preferred_element_type=jnp.float32) * SCALE
            query_parts += [unturned(back[:MB]), unturned(back[MB:])]
            key_parts.append(unturned(dot_tn(score, query) * SCALE))
        for part in range(2):
            for c, piece in enumerate(joined_heads(query_parts[part * 4 : part * 4 + 4], small)):
                column = pl.ds(pl.multiple_of(quad * 768 + part * 384 + c * 128, 128), 128)
                query_grad[band, column] = piece.astype(jnp.bfloat16)
        for parts, target in ((key_parts, key_grad), (value_parts, value_grad)):
            for c, piece in enumerate(joined_heads(parts, small)):
                column = pl.ds(pl.multiple_of(quad * 384 + c * 128, 128), 128)
                target[band, column] = piece.astype(jnp.bfloat16)
        return carry

    lax.fori_loop(0, 2 * micro, attend_back, 0)

    def project_back(j, slot):
        column = pl.ds(pl.multiple_of(j * step, step), step)
        stream_grad[:, column] = (
            dot_nt(query_grad[...], flat[slot])
            + dot_nt(key_grad[...], kv_slot[slot, 0])
            + dot_nt(value_grad[...], kv_slot[slot, 1])
        )

    streamed(width // step, 3, qkv_copies, project_back)
    norm_back(stream_grad, source, gain_one, mid, None, passed, gain_one_o, rows)

    @pl.when(section == 1)
    def _():
        for part in range(micro):
            pass_on(part).start()

    keep = loading(11, passed, out_ref)
    act_load.wait()
    staged(activated, step, incoming, flat_stage, flat_out, g_down)
    staged(ffn_input, short, gate_grad, wide_stage, wide_out, g_gate)
    staged(ffn_input, short, up_grad, wide_stage, wide_out, g_up)
    staged(attended, step, out_grad, flat_stage, flat_out, g_out)
    staged(attn_input, step, query_grad, flat_stage, flat_out, g_query)
    staged(attn_input, step, key_grad, flat_stage, flat_out, g_key)
    staged(attn_input, step, value_grad, flat_stage, flat_out, g_value)
    keep.wait()

    @pl.when(section == 1)
    def _():
        for part in range(micro):
            pass_on(part).wait_send()


def backward_call(cotangent, tables, gain_one, gain_two, weights, source, kept):
    rows, width = cotangent.shape
    micro = rows // MB
    inner = weights[4].shape[1]
    kv_width = weights[1].shape[1]
    low, full = jnp.bfloat16, jnp.float32
    S = jax.ShapeDtypeStruct
    anywhere = pl.BlockSpec(memory_space=pl.ANY)
    local = pl.BlockSpec(memory_space=pltpu.VMEM)
    V = pltpu.VMEM
    D = pltpu.SemaphoreType.DMA
    outs = pl.pallas_call(
        functools.partial(backward_kernel, rows),
        out_shape=[S((rows, width), low), S((8, width), full), S((8, width), full)]
        + [S(w.shape, low) for w in weights],
        in_specs=[anywhere] + [local] * 5 + [anywhere] * (8 + len(kept)),
        out_specs=[anywhere, local, local] + [anywhere] * 7,
        scratch_shapes=[
            V((rows, width), low), V((rows, width), low),
            V((rows, inner), low), V((rows, width), low), V((rows, width), low), V((rows, width), low), V((rows, width), low),
            V((rows, width), full), V(kept[4].shape, low), V(kept[1].shape, low), V(kept[2].shape, low), V(kept[3].shape, low),
            V((rows, inner), low), V((rows, inner), low), V((rows, width), full), V((rows, width), low), V((rows, HEADS * 128), low),
            V((rows, width), low), V((rows, kv_width), low), V((rows, kv_width), low),
            V((3, 2, rows, 512), low), V((3, 512, width), low), V((3, 2, 512, kv_width), low), V((2, 2, 256, inner), low),
            V((2, 512, width), low), V((2, 256, inner), low),
            D((3, 2)), D((3,)), D((3, 2)), D((2, 2)), D((2,)), D((2,)), D((12,)), D((micro,)), D((micro,)),
        ],
        compiler_params=pltpu.CompilerParams(collective_id=3, has_side_effects=True, vmem_limit_bytes=63 << 20),
        name="backward_layers",
    )(cotangent, *tables, gain_one, gain_two, *weights, source, *kept)
    return outs[0], outs[1].sum(axis=0), outs[2].sum(axis=0), list(outs[3:])


def shards(
    tokens, cotangent, seq_lengths, w_query, w_key, w_value, w_out, w_gate, w_up, w_down, gain_attn, gain_ffn,
):
    chips = lax.axis_size("dp") // 2
    starts = row_starts(seq_lengths, tokens.shape[0] // seq_lengths.shape[0])
    tables = padded_tables(starts)
    width = gain_attn.shape[1]
    own = [w[0] for w in (w_query, w_key, w_value, w_out, w_gate, w_up, w_down)]
    wholes = gathered(own + [packed_gains(gain_attn, gain_ffn)], chips)
    weights = wholes[:7]
    gain_one, gain_two = unpacked_gains(wholes[7], width)
    result, source, kept = forward_call(tokens, starts, tables, gain_one, gain_two, weights)
    input_grad, gain_one_grad, gain_two_grad, terms = backward_call(
        cotangent, tables, gain_one, gain_two, weights, source, kept
    )
    sums = scattered(terms + [packed_gain_sums(gain_one_grad, gain_two_grad, width)], chips)
    gains = sums[7]
    return (
        result[None],
        input_grad[None],
        *(item[None] for item in sums[:7]),
        gains[:1, :width],
        gains[:1, GAIN_LANES : GAIN_LANES + width],
    )


def solution(mesh):
    in_specs = (
        P("dp", None),
        P("dp", None),
        P("dp", None),
        P("pipe", "dp", None),
        P("pipe", "dp", None),
        P("pipe", "dp", None),
        P("pipe", "dp", None),
        P("pipe", "dp", None),
        P("pipe", "dp", None),
        P("pipe", "dp", None),
        P("pipe", "dp"),
        P("pipe", "dp"),
    )
    out_specs = (
        P("pipe", "dp", None),
        P("pipe", "dp", None),
        P("pipe", "dp", None),
        P("pipe", "dp", None),
        P("pipe", "dp", None),
        P("pipe", "dp", None),
        P("pipe", "dp", None),
        P("pipe", "dp", None),
        P("pipe", "dp", None),
        P("pipe", "dp"),
        P("pipe", "dp"),
    )
    return jax.shard_map(shards, mesh=mesh, in_specs=in_specs, out_specs=out_specs, check_vma=False)
```

```python
import functools, math
import jax
import jax.numpy as jnp
from jax import lax
from jax.experimental import pallas as pl
from jax.experimental.pallas import tpu as pltpu
from jax.sharding import PartitionSpec as P

MESH = pl.DeviceIdType.MESH
DEPTH = 4


def ring_place(dp_index, chips):
    inner = chips // DEPTH
    core = dp_index % 2
    chip = dp_index // 2
    deep = chip // inner
    spot = chip % inner
    half = inner // 2
    turn = spot + (spot // half) * (3 * half - 1 - 2 * spot)
    return turn * DEPTH + deep + (turn % 2) * (DEPTH - 1 - 2 * deep), core


def ring_device(place, core, chips):
    inner = chips // DEPTH
    half = inner // 2
    turn = place // DEPTH
    step = place % DEPTH
    deep = step + (turn % 2) * (DEPTH - 1 - 2 * step)
    spot = turn + (turn // half) * (3 * half - 1 - 2 * turn)
    return (deep * inner + spot) * 2 + core


def gather_kernel(chips, count, *refs):
    shards = refs[:count]
    wholes = refs[count : 2 * count]
    stages = refs[2 * count : 3 * count]
    ring_send, ring_recv, pair_send, pair_recv, own_pair, own_load = refs[3 * count :]
    me = lax.axis_index("dp")
    place, core = ring_place(me, chips)
    right = ring_device((place + 1) % chips, core, chips)
    left = ring_device((place + chips - 1) % chips, core, chips)
    partner = me + 1 - 2 * core
    barrier = pltpu.get_barrier_semaphore()
    for other in (right, left, partner):
        pl.semaphore_signal(barrier, inc=1, device_id={"dp": other}, device_id_type=MESH)
    pl.semaphore_wait(barrier, 3)

    def block(index, owner, way):
        rows, columns = shards[index].shape
        return wholes[index].at[
            pl.ds(pl.multiple_of(owner * rows, 8), rows), pl.ds(way * (columns // 2), columns // 2)
        ]

    def ring_copy(index, way, step, source=None):
        owner_place = (place + chips - step) % chips if way == 0 else (place + step) % chips
        owner = ring_device(owner_place, core, chips)
        target = block(index, owner, way)
        return pltpu.make_async_remote_copy(
            src_ref=target if source is None else source,
            dst_ref=target,
            send_sem=ring_send.at[index, way, step],
            recv_sem=ring_recv.at[index, way, step],
            device_id={"dp": (right, left)[way]},
            device_id_type=MESH,
        )

    def arrived(index, way, step):
        owner_place = (place + chips - step - 1) % chips if way == 0 else (place + step + 1) % chips
        owner = ring_device(owner_place, core, chips)
        target = block(index, owner, way)
        ring = pltpu.make_async_remote_copy(
            src_ref=target, dst_ref=target,
            send_sem=ring_send.at[index, way, step], recv_sem=ring_recv.at[index, way, step],
            device_id={"dp": (right, left)[way]}, device_id_type=MESH,
        )
        pair = pltpu.make_async_remote_copy(
            src_ref=target, dst_ref=target,
            send_sem=pair_send.at[index, way, step], recv_sem=pair_recv.at[index, way, step],
            device_id={"dp": partner}, device_id_type=MESH,
        )
        return ring, pair

    def own_pair_copy(index, device):
        rows = shards[index].shape[0]
        return pltpu.make_async_remote_copy(
            src_ref=shards[index],
            dst_ref=wholes[index].at[pl.ds(pl.multiple_of(device * rows, 8), rows), :],
            send_sem=own_pair.at[0, index], recv_sem=own_pair.at[1, index],
            device_id={"dp": partner}, device_id_type=MESH,
        )

    for index in range(count):
        columns = shards[index].shape[1]
        for way in range(2):
            ring_copy(index, way, 0, shards[index].at[:, pl.ds(way * (columns // 2), columns // 2)]).start()
    loads = []
    for index in range(count):
        own_pair_copy(index, me).start()
        loads.append(pltpu.make_async_copy(shards[index], stages[index], own_load.at[0, index]))
        loads[-1].start()
    stores = []
    for index in range(count):
        rows = shards[index].shape[0]
        loads[index].wait()
        stores.append(
            pltpu.make_async_copy(
                stages[index],
                wholes[index].at[pl.ds(pl.multiple_of(me * rows, 8), rows), :],
                own_load.at[1, index],
            )
        )
        stores[-1].start()

    def hop(step, carry):
        for index in range(count):
            for way in range(2):
                ring, pair = arrived(index, way, step - 1)
                ring.wait_recv()
                ring_copy(index, way, step).start()
                pair.start()
        return carry

    lax.fori_loop(1, chips - 1, hop, 0)
    for index in range(count):
        for way in range(2):
            ring, pair = arrived(index, way, chips - 2)
            ring.wait_recv()
            pair.start()

    def finish(step, carry):
        for index in range(count):
            for way in range(2):
                ring, pair = arrived(index, way, step)
                ring.wait_send()
                pair.wait_send()
                pair.wait_recv()
        return carry

    lax.fori_loop(0, chips - 1, finish, 0)
    for index in range(count):
        own_pair_copy(index, me).wait_send()
        own_pair_copy(index, partner).wait_recv()
        stores[index].wait()


def gathered(shards, chips):
    count = len(shards)
    steps = chips - 1
    return pl.pallas_call(
        functools.partial(gather_kernel, chips, count),
        out_shape=[jax.ShapeDtypeStruct((s.shape[0] * 2 * chips, s.shape[1]), s.dtype) for s in shards],
        in_specs=[pl.BlockSpec(memory_space=pl.ANY)] * count,
        out_specs=[pl.BlockSpec(memory_space=pl.ANY)] * count,
        scratch_shapes=[pltpu.VMEM(s.shape, s.dtype) for s in shards]
        + [
            pltpu.SemaphoreType.DMA((count, 2, steps)),
            pltpu.SemaphoreType.DMA((count, 2, steps)),
            pltpu.SemaphoreType.DMA((count, 2, steps)),
            pltpu.SemaphoreType.DMA((count, 2, steps)),
            pltpu.SemaphoreType.DMA((2, count)),
            pltpu.SemaphoreType.DMA((2, count)),
        ],
        compiler_params=pltpu.CompilerParams(collective_id=0, has_side_effects=True),
        name="gather_weights",
    )(*shards)


HEADS = 16
KV_HEADS = 8
HD = 96
EPSILON = 1e-05
ROPE_BASE = 100000.0
SCALE = 1.0 / math.sqrt(HD)
GAIN_LANES = 128
VMEM_MOST = 67_043_328


def row_starts(lengths, row_length):
    seq_ends = jnp.cumsum(lengths, axis=-1)
    slot_ids = jnp.arange(row_length, dtype=jnp.int32)
    reached = jnp.where(seq_ends[:, None, :] <= slot_ids[None, :, None], seq_ends[:, None, :], 0)
    return jnp.max(reached, axis=-1)


def packed_gains(first, second):
    width = first.shape[-1]
    edge = ((0, 15), (0, GAIN_LANES - width))
    return jnp.concatenate([jnp.pad(first, edge), jnp.pad(second, edge)], axis=1)


def unpacked_gains(whole, width):
    kept = whole.reshape(-1, 16, 2 * GAIN_LANES)[:, 0].astype(jnp.float32)
    return kept[:, :width].reshape(1, -1), kept[:, GAIN_LANES : GAIN_LANES + width].reshape(1, -1)


def spread_heads(tile, lane):
    first, second, third = tile[:, :128], tile[:, 128:256], tile[:, 256:384]
    return (
        first,
        jnp.where(lane < 32, pltpu.roll(first, 32, 1), pltpu.roll(second, 32, 1)),
        jnp.where(lane < 64, pltpu.roll(second, 64, 1), pltpu.roll(third, 64, 1)),
        pltpu.roll(third, 96, 1),
    )


def joined_heads(heads, lane):
    one, two, three = pltpu.roll(heads[1], 96, 1), pltpu.roll(heads[2], 64, 1), pltpu.roll(heads[3], 32, 1)
    return (
        jnp.where(lane < 96, heads[0], one),
        jnp.where(lane < 64, one, two),
        jnp.where(lane < 32, two, three),
    )


def turned(head, cosine, fore, aft):
    return head * cosine + pltpu.roll(head, 80, 1) * fore + pltpu.roll(head, 48, 1) * aft


def streamed(count, depth, copies, use):
    def body(j, carry):
        @pl.when(j + depth - 1 < count)
        def _():
            for copy in copies(j + depth - 1, (j + depth - 1) % depth):
                copy.start()

        for copy in copies(j, j % depth):
            copy.wait()
        use(j, j % depth)
        return carry

    lax.fori_loop(0, count, body, 0)


def lead(count, depth, copies):
    for j in range(min(depth - 1, count)):
        for copy in copies(j, j % depth):
            copy.start()


def normal_rows(source, target, gain, rows):
    band_rows = 64

    def body(i, carry):
        band = pl.ds(pl.multiple_of(i * band_rows, band_rows), band_rows)
        value = source[band, :].astype(jnp.float32)
        scale = lax.rsqrt(jnp.mean(value * value, axis=-1, keepdims=True) + EPSILON)
        target[band, :] = ((value * scale) * gain[...]).astype(jnp.bfloat16)
        return carry

    lax.fori_loop(0, rows // band_rows, body, 0)


def head_lane():
    return lax.broadcasted_iota(jnp.int32, (MB, 128), 1)


MB = 128
FWD_KEPT = ("attn_input", "queries", "keys", "values", "probs", "attended", "mid", "ffn_input", "gate", "up", "activated")


def forward_kernel(rows, *refs):
    (tokens, seg_column, seg_row, cosine, fore, aft, gain_one, gain_two,
     w_query, w_key, w_value, w_out, w_gate, w_up, w_down,
     out_ref, source_ref, attn_input_o, queries_o, keys_o, values_o, probs_o, attended_o, mid_o, ffn_input_o, gate_o, up_o, activated_o,
     source, result, attn_input, queries, keys, values, probs, attended, mid, ffn_input, gate, up, activated,
     square, pair_slot, tall,
     square_sem, pair_sem, tall_sem, keep_sem, load_sem, send_sem, recv_sem) = refs
    section = lax.axis_index("pipe")
    width = tokens.shape[1]
    inner = w_gate.shape[1]
    kv_width = w_key.shape[1]
    micro = rows // MB
    barrier = pltpu.get_barrier_semaphore()
    pl.semaphore_signal(barrier, inc=1, device_id={"pipe": 1 - section}, device_id_type=MESH)
    pl.semaphore_wait(barrier, 1)

    def pass_on(part):
        band = pl.ds(part * MB, MB)
        return pltpu.make_async_remote_copy(
            src_ref=result.at[band, :], dst_ref=source.at[band, :],
            send_sem=send_sem.at[part], recv_sem=recv_sem.at[part],
            device_id={"pipe": 1 - section}, device_id_type=MESH,
        )

    step = 768
    per_query = width // step
    per_kv = kv_width // step

    def qkv_copies(j):
        if j < per_query:
            weight, at = w_query, j
        elif j < per_query + per_kv:
            weight, at = w_key, j - per_query
        else:
            weight, at = w_value, j - per_query - per_kv
        return pltpu.make_async_copy(
            weight.at[:, pl.ds(at * step, step)], square.at[j % 4], square_sem.at[j % 4]
        )

    def out_copy(j):
        return pltpu.make_async_copy(
            w_out.at[:, pl.ds(j * step, step)], square.at[j % 4], square_sem.at[j % 4]
        )

    wide = 1024

    def ffn_copies(j, slot):
        column = pl.ds(pl.multiple_of(j * wide, wide), wide)
        return (
            pltpu.make_async_copy(w_gate.at[:, column], pair_slot.at[slot, 0], pair_sem.at[slot, 0]),
            pltpu.make_async_copy(w_up.at[:, column], pair_slot.at[slot, 1], pair_sem.at[slot, 1]),
        )

    narrow = 512

    def down_copies(j, slot):
        column = pl.ds(pl.multiple_of(j * narrow, narrow), narrow)
        return (pltpu.make_async_copy(w_down.at[:, column], tall.at[slot], tall_sem.at[slot]),)

    count_qkv = per_query + 2 * per_kv
    for j in range(4):
        qkv_copies(j).start()
    lead(inner // wide, 2, ffn_copies)
    lead(width // narrow, 2, down_copies)

    @pl.when(section == 0)
    def _():
        load = pltpu.make_async_copy(tokens, source, load_sem)
        load.start()
        load.wait()

    @pl.when(section == 1)
    def _():
        for part in range(micro):
            pass_on(part).wait_recv()

    kept = []

    def keep(index, here, there):
        copy = pltpu.make_async_copy(here, there, keep_sem.at[index])
        copy.start()
        kept.append(copy)

    keep(12, source, source_ref)
    normal_rows(source, attn_input, gain_one, rows)
    keep(0, attn_input, attn_input_o)
    lane = lax.broadcasted_iota(jnp.int32, (rows, 128), 1)

    def project(j):
        qkv_copies(j).wait()
        value = jnp.dot(attn_input[...], square[j % 4], preferred_element_type=jnp.float32)
        if j + 4 < count_qkv:
            qkv_copies(j + 4).start()
        elif j + 4 - count_qkv < width // step:
            pass
        return value

    for j in range(count_qkv):
        value = project(j)
        for part in range(2):
            heads = spread_heads(value[:, part * 384 : part * 384 + 384], lane)
            for k in range(4):
                if j < per_query + per_kv:
                    low = turned(heads[k], cosine[...], fore[...], aft[...]).astype(jnp.bfloat16)
                else:
                    low = jnp.where(lane < HD, heads[k], 0.0).astype(jnp.bfloat16)
                if j < per_query:
                    at, target = j * 8 + part * 4 + k, queries
                elif j < per_query + per_kv:
                    at, target = (j - per_query) * 8 + part * 4 + k, keys
                else:
                    at, target = (j - per_query - per_kv) * 8 + part * 4 + k, values
                target[:, pl.ds(at * 128, 128)] = low
    for j in range(width // step):
        out_copy(j).start()
    keep(1, queries, queries_o)
    keep(2, keys, keys_o)
    keep(3, values, values_o)

    def attend(at, carry):
        row = at // 2
        quad = at % 2
        band = pl.ds(pl.multiple_of(row * MB, MB), MB)
        slot_i = lax.broadcasted_iota(jnp.int32, (2 * MB, MB), 0)
        slot_i = jnp.where(slot_i >= MB, slot_i - MB, slot_i)
        slot_j = lax.broadcasted_iota(jnp.int32, (2 * MB, MB), 1)
        column = seg_column[band, :]
        same = jnp.concatenate([column, column], axis=0) == seg_row[pl.ds(row, 1), :]
        mask = same & (slot_j <= slot_i)
        small = head_lane()
        outs = []
        for k in range(4):
            kv = pl.ds(pl.multiple_of((quad * 4 + k) * 128, 128), 128)
            pair = quad * 8 + 2 * k
            query = jnp.concatenate(
                [
                    queries[band, pl.ds(pl.multiple_of(pair * 128, 128), 128)],
                    queries[band, pl.ds(pl.multiple_of((pair + 1) * 128, 128), 128)],
                ],
                axis=0,
            )
            scores = lax.dot_general(
                query, keys[band, kv], (((1,), (1,)), ((), ())), preferred_element_type=jnp.float32
            ) * SCALE
            scores = jnp.where(mask, scores, -1e30)
            high = jnp.max(scores, axis=-1, keepdims=True)
            grown = jnp.exp(scores - high)
            low = (grown / jnp.sum(grown, axis=-1, keepdims=True)).astype(jnp.bfloat16)
            place = pl.ds(pl.multiple_of((at * 4 + k) * 2 * MB, 2 * MB), 2 * MB)
            probs[place, :] = low
            out = jnp.dot(low, values[band, kv], preferred_element_type=jnp.float32)
            outs += [out[:MB], out[MB:]]
        for part in range(2):
            for c, piece in enumerate(joined_heads(outs[part * 4 : part * 4 + 4], small)):
                column = pl.ds(pl.multiple_of(quad * 768 + part * 384 + c * 128, 128), 128)
                attended[band, column] = piece.astype(jnp.bfloat16)
        return carry

    lax.fori_loop(0, 2 * micro, attend, 0)
    keep(4, probs, probs_o)
    keep(5, attended, attended_o)
    for j in range(width // step):
        out_copy(j).wait()
        column = pl.ds(j * step, step)
        mid[:, column] = source[:, column].astype(jnp.float32) + jnp.dot(
            attended[...], square[j % 4], preferred_element_type=jnp.float32
        )
    keep(6, mid, mid_o)
    normal_rows(mid, ffn_input, gain_two, rows)
    keep(7, ffn_input, ffn_input_o)

    def expand(j, slot):
        column = pl.ds(pl.multiple_of(j * wide, wide), wide)
        gate_part = jnp.dot(ffn_input[...], pair_slot[slot, 0], preferred_element_type=jnp.float32)
        up_part = jnp.dot(ffn_input[...], pair_slot[slot, 1], preferred_element_type=jnp.float32)
        gate[:, column] = gate_part.astype(jnp.bfloat16)
        up[:, column] = up_part.astype(jnp.bfloat16)
        activated[:, column] = (gate_part / (1.0 + jnp.exp(-gate_part)) * up_part).astype(jnp.bfloat16)

    streamed(inner // wide, 2, ffn_copies, expand)
    keep(8, gate, gate_o)
    keep(9, up, up_o)
    keep(10, activated, activated_o)

    def contract(j, slot):
        column = pl.ds(pl.multiple_of(j * narrow, narrow), narrow)
        value = mid[:, column] + jnp.dot(activated[...], tall[slot], preferred_element_type=jnp.float32)
        result[:, column] = value.astype(jnp.bfloat16)

    streamed(width // narrow, 2, down_copies, contract)
    keep(11, result, out_ref)

    @pl.when(section == 0)
    def _():
        for part in range(micro):
            pass_on(part).start()
        for part in range(micro):
            pass_on(part).wait_send()

    for copy in kept:
        copy.wait()


def forward_call(tokens, starts, tables, gain_one, gain_two, weights):
    rows, width = tokens.shape
    micro = rows // MB
    inner = weights[4].shape[1]
    kv_width = weights[1].shape[1]
    low, full = jnp.bfloat16, jnp.float32
    S = jax.ShapeDtypeStruct
    kept = [
        S((rows, width), low), S((rows, HEADS * 128), low), S((rows, KV_HEADS * 128), low), S((rows, KV_HEADS * 128), low),
        S((micro * HEADS * MB, MB), low), S((rows, width), low), S((rows, width), full), S((rows, width), low),
        S((rows, inner), low), S((rows, inner), low), S((rows, inner), low),
    ]
    anywhere = pl.BlockSpec(memory_space=pl.ANY)
    local = pl.BlockSpec(memory_space=pltpu.VMEM)
    square = 1536 // 2
    outs = pl.pallas_call(
        functools.partial(forward_kernel, rows),
        out_shape=[S((rows, width), low), S((rows, width), low)] + kept,
        in_specs=[anywhere] + [local] * 7 + [anywhere] * 7,
        out_specs=[anywhere] * (2 + len(kept)),
        scratch_shapes=[pltpu.VMEM((rows, width), low), pltpu.VMEM((rows, width), low)]
        + [pltpu.VMEM(k.shape, k.dtype) for k in kept]
        + [
            pltpu.VMEM((4, width, square), low),
            pltpu.VMEM((2, 2, width, 1024), low),
            pltpu.VMEM((2, inner, 512), low),
            pltpu.SemaphoreType.DMA((4,)),
            pltpu.SemaphoreType.DMA((2, 2)),
            pltpu.SemaphoreType.DMA((2,)),
            pltpu.SemaphoreType.DMA((13,)),
            pltpu.SemaphoreType.DMA,
            pltpu.SemaphoreType.DMA((micro,)),
            pltpu.SemaphoreType.DMA((micro,)),
        ],
        compiler_params=pltpu.CompilerParams(collective_id=2, has_side_effects=True, vmem_limit_bytes=63 << 20),
        name="forward_layers",
    )(tokens, starts.reshape(rows, 1), starts, *tables, gain_one, gain_two, *weights)
    return outs[0], outs[1], outs[2:]


def padded_tables(starts):
    places = (jnp.arange(starts.shape[1], dtype=jnp.int32)[None] - starts).astype(jnp.float32).reshape(-1, 1)
    lanes = jnp.arange(128, dtype=jnp.int32)
    half = HD // 2
    inv_freqs = jnp.exp((lanes % half).astype(jnp.float32) * (-2.0 * math.log(ROPE_BASE) / HD))
    angles = places * inv_freqs[None]
    cosine, sine = jnp.cos(angles), jnp.sin(angles)
    return (
        jnp.where(lanes < HD, cosine, 0.0),
        jnp.where(lanes < half, -sine, 0.0),
        jnp.where((lanes >= half) & (lanes < HD), sine, 0.0),
    )


def dot_nt(first, second):
    return lax.dot_general(first, second, (((1,), (1,)), ((), ())), preferred_element_type=jnp.float32)


def dot_tn(first, second):
    return lax.dot_general(first, second, (((0,), (0,)), ((), ())), preferred_element_type=jnp.float32)


def norm_back(grad, stream, gain, upper, target, low_target, gain_sum, rows):
    band_rows = 32
    gain_sum[...] = jnp.zeros_like(gain_sum)

    def body(i, carry):
        band = pl.ds(pl.multiple_of(i * band_rows, band_rows), band_rows)
        value = stream[band, :].astype(jnp.float32)
        scale = lax.rsqrt(jnp.mean(value * value, axis=-1, keepdims=True) + EPSILON)
        normed = value * scale
        term = grad[band, :] * normed
        gain_sum[...] += term.reshape(band_rows // 8, 8, term.shape[1]).sum(axis=0)
        inner_mean = jnp.mean(term * gain[...], axis=-1, keepdims=True)
        out = upper[band, :].astype(jnp.float32) + scale * (grad[band, :] * gain[...] - normed * inner_mean)
        if target is not None:
            target[band, :] = out
        low_target[band, :] = out.astype(jnp.bfloat16)
        return carry

    lax.fori_loop(0, rows // band_rows, body, 0)


class Unit:
    def __init__(self, index, piece, total, rows, columns, stage, first_column):
        self.index, self.piece, self.total, self.rows, self.columns = index, piece, total, rows, columns
        self.stage, self.first_column = stage, first_column


def backward_kernel(rows, chips, *refs):
    (cotangent, cosine, fore, aft, gain_one, gain_two,
     w_query, w_key, w_value, w_out, w_gate, w_up, w_down,
     source_i, attn_input_i, queries_i, keys_i, values_i, probs_i, attended_i, mid_i, ffn_input_i, gate_i, up_i, activated_i) = refs[:25]
    refs = refs[25:]
    out_ref, s_query, s_key, s_value, s_out, s_gate, s_up, s_down, s_gain = refs[:9]
    g_query, g_key, g_value, g_out, g_gate, g_up, g_down = refs[9:16]
    lands, arrivals = refs[16:27], refs[27:38]
    (incoming, passed, ffn_input, attn_input, attended, source, mid, probs, queries, keys, values,
     gate_grad, up_grad, stream_grad, out_grad, heads_grad, query_grad, key_grad, value_grad,
     gate_slot, flat, kv_slot, pair_slot, flat_stage,
     gate_sem, flat_sem, kv_sem, pair_sem, flat_out, wide_out, load_sem, send_sem, recv_sem,
     gain_sum_one, gain_sum_two, gain_pack,
     own_a, mate_a, sum_a, full_a, own_b, mate_b, sum_b, full_b, own_c, mate_c, sum_c, full_c,
     ring_send, ring_recv, mate_send, mate_recv, own_sem, mate_sem, sum_sem, full_sem) = refs[38:]
    section = lax.axis_index("pipe")
    width = cotangent.shape[1]
    inner = w_gate.shape[1]
    kv_width = w_key.shape[1]
    micro = rows // MB
    me = lax.axis_index("dp")
    place, core = ring_place(me, chips)
    right = ring_device((place + 1) % chips, core, chips)
    left = ring_device((place + chips - 1) % chips, core, chips)
    partner = me + 1 - 2 * core
    barrier = pltpu.get_barrier_semaphore()
    for other in (right, left, partner):
        pl.semaphore_signal(barrier, inc=1, device_id={"dp": other}, device_id_type=MESH)
    pl.semaphore_signal(barrier, inc=1, device_id={"pipe": 1 - section}, device_id_type=MESH)
    pl.semaphore_wait(barrier, 4)

    def in_rows(grad, shard_rows, columns, first_column):
        half = grad.shape[1] // 2

        def piece(device, way):
            return grad.at[
                pl.ds(pl.multiple_of(device * shard_rows, 8), shard_rows),
                pl.ds(way * half + first_column, columns),
            ]

        return piece

    units = []

    def unit(grad, total, stage, split):
        shard_rows = total.shape[0]
        columns = total.shape[1] // 2 // split
        for at in range(split):
            piece = in_rows(grad, shard_rows, columns, at * columns)
            units.append(Unit(len(units), piece, total, shard_rows, columns, stage[at], at * columns))

    bank_a = [(own_a.at[i], mate_a.at[i], sum_a.at[i], full_a) for i in range(2)]
    bank_b = [(own_b.at[i], mate_b.at[i], sum_b.at[i], full_b) for i in range(4)]
    unit(g_down, s_down, bank_a, 2)
    unit(g_gate, s_gate, bank_b[:2], 2)
    unit(g_up, s_up, bank_b[2:], 2)
    unit(g_out, s_out, bank_b[:1], 1)
    unit(g_query, s_query, bank_b[1:2], 1)
    unit(g_key, s_key, bank_b[2:3], 1)
    unit(g_value, s_value, bank_b[3:4], 1)
    units.append(
        Unit(len(units), lambda device, way: gain_pack.at[device, :, pl.ds(way * 128, 128)], s_gain, 8, 128,
             (own_c, mate_c, sum_c, full_c), 0)
    )

    def owner_chip(way, step):
        return (place + 2 * chips - 1 - step) % chips if way == 0 else (place + 1 + step) % chips

    def mate_exchange(u, way, step):
        return pltpu.make_async_remote_copy(
            src_ref=u.piece(ring_device(owner_chip(way, step), 1 - core, chips), way),
            dst_ref=lands[u.index].at[way, step],
            send_sem=mate_send.at[u.index, way, step], recv_sem=mate_recv.at[u.index, way, step],
            device_id={"dp": partner}, device_id_type=MESH,
        )

    def own_load(u, way, step):
        return pltpu.make_async_copy(
            u.piece(ring_device(owner_chip(way, step), core, chips), way),
            u.stage[0].at[way, :, pl.ds(0, u.columns)], own_sem.at[u.index, way],
        )

    def mate_load(u, way, step):
        return pltpu.make_async_copy(
            lands[u.index].at[way, step], u.stage[1].at[way, :, pl.ds(0, u.columns)], mate_sem.at[u.index, way]
        )

    def running(u, way, step):
        return u.stage[2].at[step % 2, way, :, pl.ds(0, u.columns)]

    def sum_load(u, way, step):
        return pltpu.make_async_copy(
            arrivals[u.index].at[way, step - 1], running(u, way, step), sum_sem.at[u.index, way]
        )

    def ring_copy(u, way, step):
        return pltpu.make_async_remote_copy(
            src_ref=running(u, way, step), dst_ref=arrivals[u.index].at[way, step],
            send_sem=ring_send.at[u.index, way, step], recv_sem=ring_recv.at[u.index, way, step],
            device_id={"dp": (right, left)[way]}, device_id_type=MESH,
        )

    def start_exchange(group):
        def body(step, carry):
            for u in group:
                for way in range(2):
                    mate_exchange(u, way, step).start()
            return carry

        lax.fori_loop(0, chips, body, 0)
        for u in group:
            load_terms(u, 0)

    def load_terms(u, step):
        for way in range(2):
            own_load(u, way, step).start()
            mate_exchange(u, way, step).wait_recv()
            mate_load(u, way, step).start()

    def visit(u, step, first=False, last=False):
        if not first:
            for way in range(2):
                ring_copy(u, way, step - 1).wait_recv()
                if isinstance(step, int):
                    if step >= 2:
                        ring_copy(u, way, step - 2).wait_send()
                else:

                    @pl.when(step >= 2)
                    def _():
                        ring_copy(u, way, step - 2).wait_send()

                sum_load(u, way, step).start()
        part = 32 if u.rows % 32 == 0 else 8
        for way in range(2):
            own_load(u, way, step).wait()
            mate_load(u, way, step).wait()
            if not first:
                sum_load(u, way, step).wait()
            here = running(u, way, step)
            columns = pl.ds(0, u.columns)

            def add(at, carry):
                band = pl.ds(pl.multiple_of(at * part, part), part)
                value = u.stage[0][way, band, columns].astype(jnp.float32)
                value = value + u.stage[1][way, band, columns].astype(jnp.float32)
                if not first:
                    value = value + here[band, :].astype(jnp.float32)
                if last:
                    u.stage[3][way, band, columns] = value
                else:
                    here[band, :] = value.astype(here.dtype)
                return carry

            lax.fori_loop(0, u.rows // part, add, 0)
        if last:
            puts = []
            for way in range(2):
                column = way * (u.total.shape[1] // 2) + u.first_column
                puts.append(
                    pltpu.make_async_copy(
                        u.stage[3].at[way, :, pl.ds(0, u.columns)], u.total.at[:, pl.ds(column, u.columns)], full_sem.at[way]
                    )
                )
                puts[-1].start()
            for put in puts:
                put.wait()
            for way in range(2):
                ring_copy(u, way, step - 1).wait_send()
        else:
            load_terms(u, step + 1)
            for way in range(2):
                ring_copy(u, way, step).start()

    def visits(group, step, first=False, last=False):
        for u in group:
            visit(u, step, first, last)

    down_units, gate_units, up_units, square_units, small_units = units[:2], units[2:4], units[4:6], units[6:8], units[8:]
    hops = chips - 1

    def pass_on(part):
        band = pl.ds(part * MB, MB)
        return pltpu.make_async_remote_copy(
            src_ref=passed.at[band, :], dst_ref=incoming.at[band, :],
            send_sem=send_sem.at[part], recv_sem=recv_sem.at[part],
            device_id={"pipe": 1 - section}, device_id_type=MESH,
        )

    def loading(index, there, here):
        copy = pltpu.make_async_copy(there, here, load_sem.at[index])
        copy.start()
        return copy

    mid_load = loading(1, mid_i, mid)
    rest_loads = [
        loading(2 + i, there, here)
        for i, (there, here) in enumerate(
            ((probs_i, probs), (queries_i, queries), (keys_i, keys), (values_i, values),
             (source_i, source), (ffn_input_i, ffn_input), (attn_input_i, attn_input), (attended_i, attended))
        )
    ]
    step = 512

    def flat_copy(weight, j, slot):
        return pltpu.make_async_copy(
            weight.at[pl.ds(pl.multiple_of(j * step, step), step), :], flat.at[slot], flat_sem.at[slot]
        )

    def down_copies(j, slot):
        column = pl.ds(pl.multiple_of(j * step, step), step)
        return (
            flat_copy(w_down, j, slot),
            pltpu.make_async_copy(gate_i.at[:, column], gate_slot.at[slot, 0], gate_sem.at[slot, 0]),
            pltpu.make_async_copy(up_i.at[:, column], gate_slot.at[slot, 1], gate_sem.at[slot, 1]),
        )

    def out_copies(j, slot):
        return (flat_copy(w_out, j, slot),)

    def qkv_copies(j, slot):
        band = pl.ds(pl.multiple_of(j * step, step), step)
        return (
            flat_copy(w_query, j, slot),
            pltpu.make_async_copy(w_key.at[band, :], kv_slot.at[slot, 0], kv_sem.at[slot, 0]),
            pltpu.make_async_copy(w_value.at[band, :], kv_slot.at[slot, 1], kv_sem.at[slot, 1]),
        )

    short = 256

    def ffn_copies(j, slot):
        band = pl.ds(pl.multiple_of(j * short, short), short)
        return (
            pltpu.make_async_copy(w_gate.at[band, :], pair_slot.at[slot, 0], pair_sem.at[slot, 0]),
            pltpu.make_async_copy(w_up.at[band, :], pair_slot.at[slot, 1], pair_sem.at[slot, 1]),
        )

    lead(inner // step, 3, down_copies)
    lead(width // short, 2, ffn_copies)

    @pl.when(section == 1)
    def _():
        load = loading(10, cotangent, incoming)
        load.wait()

    @pl.when(section == 0)
    def _():
        for part in range(micro):
            pass_on(part).wait_recv()

    def put_tile(stage, sems, target, j, size, columns):
        band = pl.ds(pl.multiple_of(j * size, size), size)
        return pltpu.make_async_copy(
            stage.at[j % 2, :, pl.ds(0, columns)], target.at[band, :], sems.at[j % 2]
        )

    def product_tile(left_ref, right_ref, stage, sems, target, j, size):
        columns = right_ref.shape[1]

        @pl.when(j >= 2)
        def _():
            put_tile(stage, sems, target, j - 2, size, columns).wait()

        column = pl.ds(pl.multiple_of(j * size, size), size)
        stage[j % 2, :, pl.ds(0, columns)] = dot_tn(left_ref[:, column], right_ref[...]).astype(jnp.bfloat16)
        put_tile(stage, sems, target, j, size, columns).start()

    def product_end(count, right_ref, stage, sems, target, size):
        for j in range(max(0, count - 2), count):
            put_tile(stage, sems, target, j, size, right_ref.shape[1]).wait()

    def product(left_ref, right_ref, stage, sems, target, size):
        count = left_ref.shape[1] // size

        def body(j, carry):
            product_tile(left_ref, right_ref, stage, sems, target, j, size)
            return carry

        lax.fori_loop(0, count, body, 0)
        product_end(count, right_ref, stage, sems, target, size)

    def tile_load(j):
        column = pl.ds(pl.multiple_of(j * step, step), step)
        return pltpu.make_async_copy(
            activated_i.at[:, column], gate_slot.at[2, j % 2], gate_sem.at[2, j % 2]
        )

    def down_start():
        count = inner // step
        tile_load(0).start()

        def body(j, carry):
            @pl.when(j + 1 < count)
            def _():
                tile_load(j + 1).start()

            @pl.when(j >= 2)
            def _():
                put_tile(flat_stage, flat_out, g_down, j - 2, step, width).wait()

            tile_load(j).wait()
            flat_stage[j % 2] = dot_tn(gate_slot[2, j % 2], incoming[...]).astype(jnp.bfloat16)
            put_tile(flat_stage, flat_out, g_down, j, step, width).start()
            return carry

        lax.fori_loop(0, count, body, 0)
        product_end(count, incoming, flat_stage, flat_out, g_down, step)
        start_exchange(down_units)
        visits(down_units, 0, first=True)


    def pack_gains():
        shard_width = width // (2 * chips)
        for way, sums in enumerate((gain_sum_one, gain_sum_two)):
            for device in range(2 * chips):
                offset = device * shard_width
                base = offset // 128 * 128
                if base + 128 < width:
                    span = sums[:, base : base + 256]
                    span = pltpu.roll(span, (256 - (offset - base)) % 256, 1)
                else:
                    span = sums[:, base : base + 128]
                    span = pltpu.roll(span, (128 - (offset - base)) % 128, 1)
                gain_pack[device, :, pl.ds(way * 128, 128)] = span[:, :128]

    def down_early(at, carry):
        visits(down_units, at)
        return carry

    early = min(5, hops - 1)

    def early_hop(at):
        if at <= early:

            @pl.when(section == 0)
            def _():
                visits(down_units, at)

    @pl.when(section == 0)
    def _():
        down_start()

    def contract_back(j, slot):
        column = pl.ds(pl.multiple_of(j * step, step), step)
        act_grad = dot_nt(incoming[...], flat[slot])
        gate = gate_slot[slot, 0].astype(jnp.float32)
        up = gate_slot[slot, 1].astype(jnp.float32)
        sigmoid = 1.0 / (1.0 + jnp.exp(-gate))
        gate_grad[:, column] = (act_grad * up * sigmoid * (1.0 + gate * (1.0 - sigmoid))).astype(jnp.bfloat16)
        up_grad[:, column] = (act_grad * gate * sigmoid).astype(jnp.bfloat16)

    streamed(inner // step, 3, down_copies, contract_back)
    early_hop(1)
    lead(width // step, 3, out_copies)

    def expand_back(j, slot):
        column = pl.ds(pl.multiple_of(j * short, short), short)
        stream_grad[:, column] = dot_nt(gate_grad[...], pair_slot[slot, 0]) + dot_nt(up_grad[...], pair_slot[slot, 1])

    streamed(width // short, 2, ffn_copies, expand_back)
    early_hop(2)
    mid_load.wait()
    norm_back(stream_grad, mid, gain_two, incoming, mid, out_grad, gain_sum_two, rows)
    lane = lax.broadcasted_iota(jnp.int32, (rows, 128), 1)

    def attended_back(j, slot):
        column = pl.ds(pl.multiple_of(j * step, step), step)
        stream_grad[:, column] = dot_nt(out_grad[...], flat[slot])

    streamed(width // step, 3, out_copies, attended_back)
    lead(width // step, 2, qkv_copies)
    for part in range(width // 384):
        tile = stream_grad[:, pl.ds(part * 384, 384)]
        for k, head in enumerate(spread_heads(tile, lane)):
            heads_grad[:, pl.ds((part * 4 + k) * 128, 128)] = jnp.where(lane < HD, head, 0.0).astype(jnp.bfloat16)
    for copy in rest_loads:
        copy.wait()
    early_hop(3)

    def attend_back(at, carry):
        row = at // 2
        quad = at % 2
        band = pl.ds(pl.multiple_of(row * MB, MB), MB)
        small = head_lane()
        table = (cosine[band, :], fore[band, :], aft[band, :])

        def unturned(head):
            return head * table[0] - pltpu.roll(head, 80, 1) * table[1] - pltpu.roll(head, 48, 1) * table[2]

        query_parts, key_parts, value_parts = [], [], []
        for k in range(4):
            kv = pl.ds(pl.multiple_of((quad * 4 + k) * 128, 128), 128)
            pair = quad * 8 + 2 * k
            first = pl.ds(pl.multiple_of(pair * 128, 128), 128)
            second = pl.ds(pl.multiple_of((pair + 1) * 128, 128), 128)
            query = jnp.concatenate([queries[band, first], queries[band, second]], axis=0)
            out = jnp.concatenate([heads_grad[band, first], heads_grad[band, second]], axis=0)
            low = probs[pl.ds(pl.multiple_of((at * 4 + k) * 2 * MB, 2 * MB), 2 * MB), :]
            prob_grad = dot_nt(out, values[band, kv])
            value_parts.append(dot_tn(low, out))
            full = low.astype(jnp.float32)
            score = full * (prob_grad - jnp.sum(full * prob_grad, axis=-1, keepdims=True))
            score = score.astype(jnp.bfloat16)
            back = jnp.dot(score, keys[band, kv], preferred_element_type=jnp.float32) * SCALE
            query_parts += [unturned(back[:MB]), unturned(back[MB:])]
            key_parts.append(unturned(dot_tn(score, query) * SCALE))
        for part in range(2):
            for c, piece in enumerate(joined_heads(query_parts[part * 4 : part * 4 + 4], small)):
                column = pl.ds(pl.multiple_of(quad * 768 + part * 384 + c * 128, 128), 128)
                query_grad[band, column] = piece.astype(jnp.bfloat16)
        for parts, target in ((key_parts, key_grad), (value_parts, value_grad)):
            for c, piece in enumerate(joined_heads(parts, small)):
                column = pl.ds(pl.multiple_of(quad * 384 + c * 128, 128), 128)
                target[band, column] = piece.astype(jnp.bfloat16)
        return carry

    lax.fori_loop(0, 2 * micro, attend_back, 0)
    early_hop(4)

    def project_back(j, slot):
        column = pl.ds(pl.multiple_of(j * step, step), step)
        stream_grad[:, column] = (
            dot_nt(query_grad[...], flat[slot])
            + dot_nt(key_grad[...], kv_slot[slot, 0])
            + dot_nt(value_grad[...], kv_slot[slot, 1])
        )

    streamed(width // step, 2, qkv_copies, project_back)
    norm_back(stream_grad, source, gain_one, mid, None, passed, gain_sum_one, rows)

    @pl.when(section == 1)
    def _():
        for part in range(micro):
            pass_on(part).start()

    keep = loading(11, passed, out_ref)
    early_hop(5)

    @pl.when(section == 1)
    def _():
        down_start()
        lax.fori_loop(1, early + 1, down_early, 0)
    pack_gains()
    wide_stage = pair_slot.at[0]
    product(ffn_input, gate_grad, wide_stage, wide_out, g_gate, short)
    start_exchange(gate_units)

    def down_hop(at, carry):
        visits(down_units, at)
        return carry

    lax.fori_loop(early + 1, hops, down_hop, 0)
    visits(gate_units, 0, first=True)
    visits(down_units, hops, last=True)
    wide_count = width // short

    def gate_hop(at, carry):
        visits(gate_units, at)

        @pl.when(at <= wide_count)
        def _():
            product_tile(ffn_input, up_grad, wide_stage, wide_out, g_up, at - 1, short)

        return carry

    lax.fori_loop(1, hops, gate_hop, 0)
    product_end(wide_count, up_grad, wide_stage, wide_out, g_up, short)
    start_exchange(up_units)
    visits(up_units, 0, first=True)
    visits(gate_units, hops, last=True)
    flat_count = width // step

    def up_hop(at, carry):
        visits(up_units, at)

        @pl.when(at <= flat_count)
        def _():
            product_tile(attended, out_grad, flat_stage, flat_out, g_out, at - 1, step)

        return carry

    lax.fori_loop(1, flat_count + 1, up_hop, 0)
    product_end(flat_count, out_grad, flat_stage, flat_out, g_out, step)

    def up_hop_more(at, carry):
        visits(up_units, at)

        @pl.when(at <= 2 * flat_count)
        def _():
            product_tile(attn_input, query_grad, flat_stage, flat_out, g_query, at - 1 - flat_count, step)

        return carry

    lax.fori_loop(flat_count + 1, hops, up_hop_more, 0)
    product_end(flat_count, query_grad, flat_stage, flat_out, g_query, step)
    start_exchange(square_units)
    visits(square_units, 0, first=True)
    product(attn_input, key_grad, flat_stage, flat_out, g_key, step)
    product(attn_input, value_grad, flat_stage, flat_out, g_value, step)
    visits(up_units, hops, last=True)
    start_exchange(small_units)
    visits(small_units, 0, first=True)

    def last_hop(at, carry):
        visits(square_units, at)
        visits(small_units, at)
        return carry

    lax.fori_loop(1, hops, last_hop, 0)
    visits(square_units, hops, last=True)
    visits(small_units, hops, last=True)
    keep.wait()

    def settle(at, carry):
        for u in units:
            for way in range(2):
                mate_exchange(u, way, at).wait_send()
        return carry

    lax.fori_loop(0, chips, settle, 0)

    @pl.when(section == 1)
    def _():
        for part in range(micro):
            pass_on(part).wait_send()


def backward_call(cotangent, tables, gain_one, gain_two, weights, source, kept, chips):
    rows, width = cotangent.shape
    micro = rows // MB
    inner = weights[4].shape[1]
    kv_width = weights[1].shape[1]
    low, full = jnp.bfloat16, jnp.float32
    S = jax.ShapeDtypeStruct
    anywhere = pl.BlockSpec(memory_space=pl.ANY)
    local = pl.BlockSpec(memory_space=pltpu.VMEM)
    V = pltpu.VMEM
    D = pltpu.SemaphoreType.DMA
    shards_n = 2 * chips
    sums = [S((w.shape[0] // shards_n, w.shape[1]), full) for w in weights] + [S((8, 256), full)]
    pieces = [(inner // shards_n, width // 4, low)] * 2 + [(width // shards_n, inner // 4, low)] * 4
    pieces += [(width // shards_n, width // 2, low)] * 2 + [(width // shards_n, kv_width // 2, low)] * 2 + [(8, 128, full)]
    count = len(pieces)
    tall, slim = inner // shards_n, width // shards_n
    quarter, wide = width // 4, inner // 4
    outs = pl.pallas_call(
        functools.partial(backward_kernel, rows, chips),
        out_shape=[S((rows, width), low)] + sums + [S(w.shape, low) for w in weights]
        + [S((2, chips, r, c), k) for r, c, k in pieces] + [S((2, chips - 1, r, c), k) for r, c, k in pieces],
        in_specs=[anywhere] + [local] * 5 + [anywhere] * (8 + len(kept)),
        out_specs=[anywhere] * (1 + len(sums) + 7 + 2 * count),
        scratch_shapes=[
            V((rows, width), low), V((rows, width), low),
            V((rows, width), low), V((rows, width), low), V((rows, width), low), V((rows, width), low),
            V((rows, width), full), V(kept[4].shape, low), V(kept[1].shape, low), V(kept[2].shape, low), V(kept[3].shape, low),
            V((rows, inner), low), V((rows, inner), low), V((rows, width), full), V((rows, width), low), V((rows, HEADS * 128), low),
            V((rows, width), low), V((rows, kv_width), low), V((rows, kv_width), low),
            V((3, 2, rows, 512), low), V((3, 512, width), low), V((2, 2, 512, kv_width), low), V((2, 2, 256, inner), low),
            V((2, 512, width), low),
            D((3, 2)), D((3,)), D((3, 2)), D((2, 2)), D((2,)), D((2,)), D((12,)), D((micro,)), D((micro,)),
            V((8, width), full), V((8, width), full), V((shards_n, 8, 256), full),
            V((2, 2, tall, quarter), low), V((2, 2, tall, quarter), low), V((2, 2, 2, tall, quarter), low), V((2, tall, quarter), full),
            V((4, 2, slim, wide), low), V((4, 2, slim, wide), low), V((4, 2, 2, slim, wide), low), V((2, slim, wide), full),
            V((2, 8, 128), full), V((2, 8, 128), full), V((2, 2, 8, 128), full), V((2, 8, 128), full),
            D((count, 2, chips - 1)), D((count, 2, chips - 1)), D((count, 2, chips)), D((count, 2, chips)),
            D((count, 2)), D((count, 2)), D((count, 2)), D((2,)),
        ],
        compiler_params=pltpu.CompilerParams(collective_id=3, has_side_effects=True, vmem_limit_bytes=VMEM_MOST),
        name="backward_layers",
    )(cotangent, *tables, gain_one, gain_two, *weights, source, *kept)
    return outs[0], outs[1 : 1 + len(sums)]


def shards(
    tokens, cotangent, seq_lengths, w_query, w_key, w_value, w_out, w_gate, w_up, w_down, gain_attn, gain_ffn,
):
    chips = lax.axis_size("dp") // 2
    starts = row_starts(seq_lengths, tokens.shape[0] // seq_lengths.shape[0])
    tables = padded_tables(starts)
    width = gain_attn.shape[1]
    own = [w[0] for w in (w_query, w_key, w_value, w_out, w_gate, w_up, w_down)]
    wholes = gathered(own + [packed_gains(gain_attn, gain_ffn)], chips)
    weights = wholes[:7]
    gain_one, gain_two = unpacked_gains(wholes[7], width)
    result, source, kept = forward_call(tokens, starts, tables, gain_one, gain_two, weights)
    input_grad, sums = backward_call(cotangent, tables, gain_one, gain_two, weights, source, kept, chips)
    gains = sums[7].sum(axis=0, keepdims=True)
    return (
        result[None],
        input_grad[None],
        *(item[None] for item in sums[:7]),
        gains[:, :width],
        gains[:, GAIN_LANES : GAIN_LANES + width],
    )


def solution(mesh):
    in_specs = (
        P("dp", None),
        P("dp", None),
        P("dp", None),
        P("pipe", "dp", None),
        P("pipe", "dp", None),
        P("pipe", "dp", None),
        P("pipe", "dp", None),
        P("pipe", "dp", None),
        P("pipe", "dp", None),
        P("pipe", "dp", None),
        P("pipe", "dp"),
        P("pipe", "dp"),
    )
    out_specs = (
        P("pipe", "dp", None),
        P("pipe", "dp", None),
        P("pipe", "dp", None),
        P("pipe", "dp", None),
        P("pipe", "dp", None),
        P("pipe", "dp", None),
        P("pipe", "dp", None),
        P("pipe", "dp", None),
        P("pipe", "dp", None),
        P("pipe", "dp"),
        P("pipe", "dp"),
    )
    return jax.shard_map(shards, mesh=mesh, in_specs=in_specs, out_specs=out_specs, check_vma=False)
```
